128 devices in a mesh: tm: 32 (over y_lo, x, z), space: 4 (over y_hi, core).
Axes of the slice: x: 4, y: 4 (y_hi: 2, y_lo: 2; y = y_hi * 2 + y_lo), z: 4, core: 2. Of those that a mesh axis runs over, the one named last changes fastest.
Arguments:
- start_block: float32 [32, 2, 3, 32, 32, 256], P('tm', None, None, None, 'space'), may hold values from -6 to 6
- gauge_links: float32 [32, 3, 2, 3, 3, 32, 256], P('tm', None, None, None, None, 'space'), may hold values from -1 to 1, as said below
- stored_vectors: bfloat16 [32, 448, 2, 3, 32, 256], P('tm', None, None, None, 'space'), may hold values from -0.02734375 to 0.02734375
Outputs:
- correlations: float32 [32, 448, 64], P('tm', 'space')
- solver_blocks: bfloat16 [32, 32, 256, 192], P('space', None, 'tm')
The draws below stay inside these ranges and needn't reach their ends.
Inputs may be any that keep to these rules, and one draw needn't show every extreme that they name: Every link matrix gauge_links[t, mu, 0] + i gauge_links[t, mu, 1] at a site is special unitary, drawn independently at every site and direction.
All inputs are finite; a program needn't handle non-finite values.
Results may differ from the reference program's by a relative error of at most 0.0029.
Values may be sent and summed in bfloat16 or wider, within the bound.
A program may use at most 128 MiB of HBM per device.

```python
import jax
import jax.numpy as jnp
from jax import lax

NVEC = 32
NSTORE = 448
DEGREE = 4
LY = 16
LZ = 16
NX = 32
LYZ = 256
NT = 32


def draw_gauge_links(key, part):
    keys = jax.random.split(jax.random.fold_in(key, 17), 2)
    shape = (3, 3, NT, 3, NX, LY * LZ)
    real_part = jax.random.uniform(keys[0], shape, jnp.float32, -1.0, 1.0)
    imag_part = jax.random.uniform(keys[1], shape, jnp.float32, -1.0, 1.0)
    real_part = real_part + 3.0 * jnp.eye(3, dtype=jnp.float32)[:, :, None, None, None, None]
    first_re, first_im = (real_part[0], imag_part[0])
    second_re, second_im = (real_part[1], imag_part[1])
    first_scale = lax.rsqrt(jnp.sum(first_re * first_re + first_im * first_im, axis=0) + 1e-12)
    first_re = first_re * first_scale
    first_im = first_im * first_scale
    proj_re = jnp.sum(first_re * second_re + first_im * second_im, axis=0)
    proj_im = jnp.sum(first_re * second_im - first_im * second_re, axis=0)
    second_re = second_re - (proj_re * first_re - proj_im * first_im)
    second_im = second_im - (proj_re * first_im + proj_im * first_re)
    second_scale = lax.rsqrt(jnp.sum(second_re * second_re + second_im * second_im, axis=0) + 1e-12)
    second_re = second_re * second_scale
    second_im = second_im * second_scale

    def product_re(col_a, col_b):
        return first_re[col_a] * second_re[col_b] - first_im[col_a] * second_im[col_b]

    def product_im(col_a, col_b):
        return first_re[col_a] * second_im[col_b] + first_im[col_a] * second_re[col_b]
    third_re = jnp.stack([product_re(1, 2) - product_re(2, 1), product_re(2, 0) - product_re(0, 2), product_re(0, 1) - product_re(1, 0)], axis=0)
    third_im = -jnp.stack([product_im(1, 2) - product_im(2, 1), product_im(2, 0) - product_im(0, 2), product_im(0, 1) - product_im(1, 0)], axis=0)
    rows_re = jnp.stack([first_re, second_re, third_re], axis=0)
    rows_im = jnp.stack([first_im, second_im, third_im], axis=0)
    stacked = jnp.stack([rows_re, rows_im], axis=0)
    return jnp.transpose(stacked, (3, 4, 0, 1, 2, 5, 6)).astype(jnp.float32)


def steps_of(rng, extent, cuts, low, largest):
    def one(axis_at, shards_of):
        draws = jax.random.uniform(jax.random.fold_in(jax.random.fold_in(rng, 6), axis_at), (shards_of,), jnp.float32, low / len(cuts), largest / len(cuts))
        return jnp.repeat(jnp.exp(draws), extent[axis_at] // shards_of).reshape((-1,) + (1,) * (len(extent) - axis_at - 1))

    factor_of = one(*cuts[0])
    for cut in cuts[1:]:
        factor_of = factor_of * one(*cut)
    return factor_of


def normal_values(rng, extent, scale, limit, shards=(), kind=jnp.bfloat16):
    loudness = steps_of(rng, extent, shards, -0.22, 0.18) if shards else 1.0
    entries = jax.random.normal(rng, extent, jnp.float32) * scale * loudness
    return jnp.minimum(jnp.maximum(entries, -limit), limit).astype(kind)


def setup_inputs(seed: int = 0) -> dict:
    streams_of = jax.random.split(jax.random.key(seed), 4)
    start_block = normal_values(streams_of[0], (NT, 2, 3, NVEC, NX, LYZ), 1.0, 6.0, ((0, 32), (4, 4)), jnp.float32)
    gauge_links = draw_gauge_links(jax.random.fold_in(streams_of[3], 71), 0)
    stored_vectors = normal_values(streams_of[2], (NT, NSTORE, 2, 3, NX, LYZ), (6 * NX * LYZ) ** -0.5, 0.02734375, ((0, 32), (4, 4)))
    return {"start_block": start_block, "gauge_links": gauge_links, "stored_vectors": stored_vectors}


lower_edge = 0.5
upper_edge = 12.5


def contract(matrix, vector):
    return jnp.sum(matrix[:, :, :, None] * vector[:, None], axis=2)


def complex_apply(link, source):
    link_re, link_im = link[:, 0], link[:, 1]
    src_re, src_im = source[:, 0], source[:, 1]
    out_re = contract(link_re, src_re) - contract(link_im, src_im)
    out_im = contract(link_re, src_im) + contract(link_im, src_re)
    return jnp.stack([out_re, out_im], axis=1)


def dagger(link):
    return jnp.stack([jnp.swapaxes(link[:, 0], 1, 2), -jnp.swapaxes(link[:, 1], 1, 2)], axis=1)


def z_forward(values):
    along_z = lax.broadcasted_iota(jnp.int32, values.shape, values.ndim - 1) % LZ
    return jnp.where(along_z == LZ - 1, jnp.roll(values, LZ - 1, axis=-1), jnp.roll(values, -1, axis=-1))


def z_backward(values):
    along_z = lax.broadcasted_iota(jnp.int32, values.shape, values.ndim - 1) % LZ
    return jnp.where(along_z == 0, jnp.roll(values, -(LZ - 1), axis=-1), jnp.roll(values, 1, axis=-1))


def laplace_interior(source, links):
    center = source[..., 1:-1, :]
    inner_links = links[..., 1:-1, :]
    link_y = inner_links[:, 1]
    link_z = inner_links[:, 2]
    hopping = complex_apply(inner_links[:, 0], source[..., 2:, :])
    hopping = hopping + complex_apply(dagger(links[:, 0, ..., :-2, :]), source[..., :-2, :])
    hopping = hopping + complex_apply(link_y, jnp.roll(center, -LZ, axis=-1))
    hopping = hopping + complex_apply(dagger(jnp.roll(link_y, LZ, axis=-1)), jnp.roll(center, LZ, axis=-1))
    hopping = hopping + complex_apply(link_z, z_forward(center))
    hopping = hopping + complex_apply(dagger(z_backward(link_z)), z_backward(center))
    return 6.0 * center - hopping


def cheb_apply(source, links):
    scale_term = 2.0 / (upper_edge - lower_edge)
    offset_term = (upper_edge + lower_edge) / (upper_edge - lower_edge)
    return scale_term * laplace_interior(source, links) - offset_term * source[..., 1:-1, :]


def wrap_pad(values):
    return jnp.concatenate([values[..., -1:, :], values, values[..., :1, :]], axis=-2)


def filter_slice(inputs):
    block_slice, link_slice = inputs
    link_pad = wrap_pad(link_slice[None])
    prev_term = block_slice[None]
    this_term = cheb_apply(wrap_pad(prev_term), link_pad)
    for level in range(1, DEGREE):
        next_term = 2.0 * cheb_apply(wrap_pad(this_term), link_pad) - prev_term
        prev_term, this_term = this_term, next_term
    return this_term[0]


def correlation_slice(inputs):
    stored_slice, half_slice = inputs
    vectors = half_slice.astype(jnp.float32)
    turned = jnp.stack([vectors[1], -vectors[0]], axis=0)
    stacked = jnp.stack([vectors, turned], axis=0)
    result = jnp.einsum("srcxy,prcvxy->spv", stored_slice.astype(jnp.float32), stacked, precision=lax.Precision.HIGHEST)
    return result.reshape(NSTORE, 2 * NVEC)


def reference(start_block, gauge_links, stored_vectors):
    filtered = lax.map(filter_slice, (start_block, gauge_links))
    filtered_half = filtered.astype(jnp.bfloat16)
    correlations = lax.map(correlation_slice, (stored_vectors, filtered_half))
    solver_blocks = jnp.transpose(filtered_half, (0, 4, 5, 1, 2, 3)).reshape(NT, NX, LYZ, 6 * NVEC)
    return correlations, solver_blocks
```

```python
import jax
import jax.numpy as jnp
from jax import lax
from jax.experimental import pallas as pl
from jax.experimental.pallas import tpu as pltpu
from jax.sharding import PartitionSpec as P

F32 = jnp.float32
BF16 = jnp.bfloat16

NVEC = 32
LZ = 16
LAYERS = 8
HALVES = 2
LANES = 128
PC = 6
ROWS = 24
FIRST = 8
LAST = 15
BELOW = 7
ABOVE = 16
BATCHES = 8
PER_BATCH = NVEC // BATCHES
HALO_ROWS = PC * PER_BATCH * HALVES
APPLICATIONS = 4
STORE_BLOCK = 32


def lane_index():
    return lax.broadcasted_iota(jnp.int32, (LAYERS, LANES), 1)


def y_forward(low, high):
    lane = lane_index()
    a, b = pltpu.roll(low, LANES - LZ, 1), pltpu.roll(high, LANES - LZ, 1)
    keep = lane < LANES - LZ
    return jnp.where(keep, a, b), jnp.where(keep, b, a)


def y_backward(low, high):
    lane = lane_index()
    a, b = pltpu.roll(low, LZ, 1), pltpu.roll(high, LZ, 1)
    keep = lane >= LZ
    return jnp.where(keep, a, b), jnp.where(keep, b, a)


def z_forward(tile):
    along_z = lane_index() % LZ
    return jnp.where(along_z == LZ - 1, pltpu.roll(tile, LZ - 1, 1), pltpu.roll(tile, LANES - 1, 1))


def z_backward(tile):
    along_z = lane_index() % LZ
    return jnp.where(along_z == 0, pltpu.roll(tile, LANES - LZ + 1, 1), pltpu.roll(tile, 1, 1))


def kernel(
    start_ref, links_ref, stored_ref, corr_ref, solver_ref,
    x_buf, a_buf, b_buf, raw, coef, top_send, top_recv, halo_send, halo_recv,
    stored, blocks, turned, product, part_send, part_recv,
    in_sem, stored_sem, top_sem, halo_send_sem, halo_recv_sem,
    block_send_sem, block_recv_sem, own_sem, part_send_sem, part_recv_sem,
):
    me_t = lax.axis_index("tm")
    me_s = lax.axis_index("space")
    up = lax.rem(me_s + 1, 4)
    down = lax.rem(me_s + 3, 4)
    target_space = me_t // 8
    source_first = me_s * 8
    has_self = target_space == me_s

    copies_in = []
    for h in range(HALVES):
        lanes = pl.ds(h * LANES, LANES)
        copies_in.append(pltpu.make_async_copy(
            start_ref.at[:, :, :, :, lanes],
            x_buf.at[:, :, :, h, pl.ds(FIRST, LAYERS), :],
            in_sem.at[h],
        ))
        copies_in.append(pltpu.make_async_copy(
            links_ref.at[:, :, :, :, lanes],
            raw.at[:, :, :, h, pl.ds(FIRST, LAYERS), :],
            in_sem.at[2 + h],
        ))
    for copy in copies_in:
        copy.start()
    stored_copy = pltpu.make_async_copy(stored_ref, stored, stored_sem)
    stored_copy.start()

    barrier = pltpu.get_barrier_semaphore()
    for step in range(1, 4):
        pl.semaphore_signal(barrier, inc=1, device_id={"space": lax.rem(me_s + step, 4)}, device_id_type=pl.DeviceIdType.MESH)

    def greet(i, carry):
        tm_of = source_first + i // 4
        space_of = lax.rem(i, 4)

        @pl.when(jnp.logical_not(jnp.logical_and(tm_of == me_t, space_of == me_s)))
        def _():
            pl.semaphore_signal(barrier, inc=1, device_id=(tm_of, space_of), device_id_type=pl.DeviceIdType.MESH)

        return carry

    lax.fori_loop(0, 32, greet, 0)

    copies_in[1].wait()
    copies_in[3].wait()

    raw_rows = raw.reshape(54 * HALVES * ROWS, LANES)
    top_send[...] = raw_rows[pl.ds(LAST, 36, stride=ROWS), :]

    pl.semaphore_wait(barrier, 35 - has_self.astype(jnp.int32))

    top_copy = pltpu.make_async_remote_copy(
        top_send, top_recv, top_sem.at[0], top_sem.at[1],
        device_id={"space": up}, device_id_type=pl.DeviceIdType.MESH,
    )
    top_copy.start()

    def halo_copy(level, side, batch):
        return pltpu.make_async_remote_copy(
            halo_send.at[level, side, batch],
            halo_recv.at[level, side, batch],
            halo_send_sem.at[level, side, batch],
            halo_recv_sem.at[level, side, batch],
            device_id={"space": up if side else down},
            device_id_type=pl.DeviceIdType.MESH,
        )

    def flat(buf):
        return buf.reshape(PC * NVEC * HALVES * ROWS, LANES)

    def send_halo(level, buf, batch):
        rows = flat(buf)
        for side in range(2):
            row = LAST if side else FIRST
            pieces = []
            for pc in range(PC):
                base = ((pc * NVEC + batch * PER_BATCH) * HALVES) * ROWS + row
                pieces.append(rows[pl.ds(base, PER_BATCH * HALVES, stride=ROWS), :])
            halo_send[level, side, batch] = jnp.concatenate(pieces, axis=0).astype(BF16)
            halo_copy(level, side, batch).start()

    def take_halo(level, buf, batch):
        rows = flat(buf)
        for side in range(2):
            row = BELOW if side else ABOVE
            halo_copy(level, side, batch).wait_recv()
            values = halo_recv[level, side, batch].astype(F32)
            for pc in range(PC):
                base = ((pc * NVEC + batch * PER_BATCH) * HALVES) * ROWS + row
                count = PER_BATCH * HALVES
                rows[pl.ds(base, count, stride=ROWS), :] = values[pc * count:(pc + 1) * count]

    copies_in[0].wait()
    copies_in[2].wait()

    def first_halo(batch, carry):
        send_halo(0, x_buf, batch)
        return carry

    lax.fori_loop(0, BATCHES, first_halo, 0)

    def put(direction, entry, half, re, im):
        coef[direction, entry, 0, half] = re
        coef[direction, entry, 1, half] = im - re
        coef[direction, entry, 2, half] = re + im

    def centre(d, part, entry, half):
        return raw[d, part, entry, half, FIRST:FIRST + LAYERS, :]

    def prepare(entry, carry):
        mirrored = lax.rem(entry, 3) * 3 + entry // 3
        for d in range(3):
            for half in range(HALVES):
                put(2 * d, entry, half, centre(d, 0, entry, half), centre(d, 1, entry, half))
        low = y_backward(centre(1, 0, entry, 0), centre(1, 0, entry, 1))
        high = y_backward(centre(1, 1, entry, 0), centre(1, 1, entry, 1))
        for half in range(HALVES):
            put(3, mirrored, half, low[half], -high[half])
            put(5, mirrored, half, z_backward(centre(2, 0, entry, half)), -z_backward(centre(2, 1, entry, half)))
        return carry

    lax.fori_loop(0, 9, prepare, 0)

    top_copy.wait_recv()
    raw_rows[pl.ds(BELOW, 36, stride=ROWS), :] = top_recv[...]

    def prepare_below(entry, carry):
        mirrored = lax.rem(entry, 3) * 3 + entry // 3
        for half in range(HALVES):
            re = raw[0, 0, entry, half, pl.ds(BELOW, LAYERS), :]
            im = raw[0, 1, entry, half, pl.ds(BELOW, LAYERS), :]
            put(1, mirrored, half, re, -im)
        return carry

    lax.fori_loop(0, 9, prepare_below, 0)

    def hop_sums(src, v):
        sums = [[None] * 9 for _ in range(HALVES)]

        def add(direction, half, parts):
            for row in range(3):
                for col in range(3):
                    re, im = parts[col], parts[3 + col]
                    for kind, value in enumerate((parts[6 + col], re, im)):
                        term = coef[direction, row * 3 + col, kind, half] * value
                        at = row * 3 + kind
                        sums[half][at] = term if sums[half][at] is None else sums[half][at] + term

        def extended(parts):
            return parts + [parts[c] + parts[3 + c] for c in range(3)]

        own = [[src[pc // 3, pc % 3, v, half, FIRST:FIRST + LAYERS, :] for pc in range(PC)] for half in range(HALVES)]
        for half in range(HALVES):
            add(0, half, extended([src[pc // 3, pc % 3, v, half, pl.ds(FIRST + 1, LAYERS), :] for pc in range(PC)]))
            add(1, half, extended([src[pc // 3, pc % 3, v, half, pl.ds(FIRST - 1, LAYERS), :] for pc in range(PC)]))
        for direction, shift in ((2, y_forward), (3, y_backward)):
            moved = [shift(own[0][pc], own[1][pc]) for pc in range(PC)]
            for half in range(HALVES):
                add(direction, half, extended([m[half] for m in moved]))
        for direction, shift in ((4, z_forward), (5, z_backward)):
            for half in range(HALVES):
                add(direction, half, extended([shift(own[half][pc]) for pc in range(PC)]))
        out = []
        for half in range(HALVES):
            s = sums[half]
            re = [s[3 * r] - s[3 * r + 2] + 0.5 * own[half][r] for r in range(3)]
            im = [s[3 * r] + s[3 * r + 1] + 0.5 * own[half][3 + r] for r in range(3)]
            out.append(re + im)
        return out

    def apply(level, src, dst):
        def one(v, carry):
            out = hop_sums(src, v)
            for half in range(HALVES):
                for pc in range(PC):
                    value = out[half][pc]
                    at = (pc // 3, pc % 3, v, half, slice(FIRST, FIRST + LAYERS), slice(None))
                    if level == 1:
                        value = value - 36.0 * x_buf[at]
                    if level == 3:
                        value = value * (1.0 / 162.0) + x_buf[at]
                    dst[at] = value
            return carry

        def batch_step(batch, carry):
            take_halo(level, src, batch)
            lax.fori_loop(batch * PER_BATCH, (batch + 1) * PER_BATCH, one, 0)
            if level + 1 < APPLICATIONS:
                send_halo(level + 1, dst, batch)
            return carry

        lax.fori_loop(0, BATCHES, batch_step, 0)

    apply(0, x_buf, a_buf)
    apply(1, a_buf, b_buf)
    apply(2, b_buf, a_buf)
    apply(3, a_buf, b_buf)

    result_rows = flat(b_buf)

    def arrange(layer, carry):
        for half in range(HALVES):
            lanes = slice(half * LANES, (half + 1) * LANES)
            pieces = []
            for pc in range(PC):
                base = (pc * NVEC * HALVES + half) * ROWS + FIRST + layer
                pieces.append(rows_of(base))
            whole = jnp.concatenate(pieces, axis=0)
            sites = whole.T.astype(BF16)
            blocks[half * 16:(half + 1) * 16, layer] = sites.reshape(16, 8, PC * NVEC)
            for c in range(3):
                re, im = pieces[c].astype(BF16), pieces[3 + c].astype(BF16)
                at = pl.ds(pl.multiple_of(layer * 64, 64), 64)
                turned[at, c * 256 + half * LANES:c * 256 + (half + 1) * LANES] = jnp.concatenate([re, im], axis=0)
                turned[at, (3 + c) * 256 + half * LANES:(3 + c) * 256 + (half + 1) * LANES] = jnp.concatenate([im, -re], axis=0)
        return carry

    def rows_of(base):
        return result_rows[pl.ds(base, NVEC, stride=HALVES * ROWS), :]

    lax.fori_loop(0, LAYERS, arrange, 0)

    target_rows = pl.ds(me_s * LAYERS, LAYERS)
    local_t = lax.rem(me_t, 8)

    def block_copy(tm_of):
        return pltpu.make_async_remote_copy(
            blocks.at[tm_of],
            solver_ref.at[local_t, target_rows],
            block_send_sem.at[tm_of],
            block_recv_sem.at[local_t * 4 + me_s],
            device_id=(tm_of, target_space),
            device_id_type=pl.DeviceIdType.MESH,
        )

    own_copy = pltpu.make_async_copy(blocks.at[me_t], solver_ref.at[local_t, target_rows], own_sem)

    @pl.when(has_self)
    def _():
        own_copy.start()

    def send_block(i, carry):
        tm_of = lax.rem(me_t + i, 32)

        @pl.when(jnp.logical_or(i > 0, jnp.logical_not(has_self)))
        def _():
            block_copy(tm_of).start()

        return carry

    lax.fori_loop(0, 32, send_block, 0)

    stored_copy.wait()

    def correlate(block, carry):
        first = pl.multiple_of(block * STORE_BLOCK, STORE_BLOCK)
        some = [stored[pl.ds(first, STORE_BLOCK), rc].reshape(STORE_BLOCK * LAYERS, 256) for rc in range(PC)]
        left = jnp.concatenate(some, axis=1)
        product[...] = lax.dot_general(
            left, turned[...], (((1,), (1,)), ((), ())), preferred_element_type=F32
        )
        layer = lax.broadcasted_iota(jnp.int32, (STORE_BLOCK * LAYERS, LANES), 0) % LAYERS
        upper = lax.broadcasted_iota(jnp.int32, (STORE_BLOCK * LAYERS, LANES), 1) // 64
        total = jnp.zeros((STORE_BLOCK * LAYERS, LANES), F32)
        for pair in range(4):
            total = jnp.where(layer == 2 * pair + upper, product[:, pair * LANES:(pair + 1) * LANES], total)
        summed = jnp.sum(total.reshape(STORE_BLOCK, LAYERS, LANES), axis=1)
        part_send[pl.ds(first, STORE_BLOCK), :] = summed
        return carry

    lax.fori_loop(0, 448 // STORE_BLOCK, correlate, 0)

    def part_copy(step):
        other = lax.rem(me_s + step, 4)
        return pltpu.make_async_remote_copy(
            part_send.at[pl.ds(pl.multiple_of(other * 112, 8), 112)],
            part_recv.at[step - 1],
            part_send_sem.at[step - 1],
            part_recv_sem.at[step - 1],
            device_id={"space": other},
            device_id_type=pl.DeviceIdType.MESH,
        )

    for step in range(1, 4):
        part_copy(step).start()
    total = part_send[pl.ds(pl.multiple_of(me_s * 112, 8), 112), :]
    for step in range(1, 4):
        part_copy(step).wait_recv()
        total = total + part_recv[step - 1]
    folded = total[:, :64] + total[:, 64:]
    corr_ref[...] = folded.T

    def finish_halo(i, carry):
        for level in range(APPLICATIONS):
            for side in range(2):
                halo_copy(level, side, i).wait_send()
        return carry

    lax.fori_loop(0, BATCHES, finish_halo, 0)
    top_copy.wait_send()
    for step in range(1, 4):
        part_copy(step).wait_send()

    @pl.when(has_self)
    def _():
        own_copy.wait()

    def finish_block(i, carry):
        tm_of = lax.rem(me_t + i, 32)

        @pl.when(jnp.logical_or(i > 0, jnp.logical_not(has_self)))
        def _():
            block_copy(tm_of).wait_send()

        return carry

    lax.fori_loop(0, 32, finish_block, 0)

    def take_block(i, carry):
        tm_of = source_first + i // 4
        space_of = lax.rem(i, 4)

        @pl.when(jnp.logical_not(jnp.logical_and(tm_of == me_t, space_of == me_s)))
        def _():
            pltpu.make_async_remote_copy(
                blocks.at[0],
                solver_ref.at[i // 4, pl.ds(space_of * LAYERS, LAYERS)],
                block_send_sem.at[0],
                block_recv_sem.at[i],
                device_id=(tm_of, space_of),
                device_id_type=pl.DeviceIdType.MESH,
            ).wait_recv()

        return carry

    lax.fori_loop(0, 32, take_block, 0)


def shards(start_block, gauge_links, stored_vectors):
    any_space = pl.BlockSpec(memory_space=pl.ANY)
    buffer = pltpu.VMEM((2, 3, NVEC, HALVES, ROWS, LANES), F32)
    halo = pltpu.VMEM((APPLICATIONS, 2, BATCHES, HALO_ROWS, LANES), BF16)
    halo_sem = pltpu.SemaphoreType.DMA((APPLICATIONS, 2, BATCHES))
    corr, solver = pl.pallas_call(
        kernel,
        out_shape=(
            jax.ShapeDtypeStruct((64, 112), F32),
            jax.ShapeDtypeStruct((8, 32, 8, 192), BF16),
        ),
        in_specs=[any_space] * 3,
        out_specs=(pl.BlockSpec(memory_space=pltpu.VMEM), any_space),
        scratch_shapes=[
            buffer, buffer, buffer,
            pltpu.VMEM((3, 2, 9, HALVES, ROWS, LANES), F32),
            pltpu.VMEM((6, 9, 3, HALVES, LAYERS, LANES), F32),
            pltpu.VMEM((36, LANES), F32),
            pltpu.VMEM((36, LANES), F32),
            halo, halo,
            pltpu.VMEM((448, 6, LAYERS, 256), BF16),
            pltpu.VMEM((32, LAYERS, 8, 192), BF16),
            pltpu.VMEM((512, 1536), BF16),
            pltpu.VMEM((STORE_BLOCK * LAYERS, 512), F32),
            pltpu.VMEM((448, LANES), F32),
            pltpu.VMEM((3, 112, LANES), F32),
            pltpu.SemaphoreType.DMA((4,)),
            pltpu.SemaphoreType.DMA,
            pltpu.SemaphoreType.DMA((2,)),
            halo_sem, halo_sem,
            pltpu.SemaphoreType.DMA((32,)),
            pltpu.SemaphoreType.DMA((32,)),
            pltpu.SemaphoreType.DMA,
            pltpu.SemaphoreType.DMA((3,)),
            pltpu.SemaphoreType.DMA((3,)),
        ],
        compiler_params=pltpu.CompilerParams(
            collective_id=0, has_side_effects=True, vmem_limit_bytes=60 * 1024 * 1024
        ),
    )(
        start_block[0],
        gauge_links[0].reshape(3, 2, 9, LAYERS, 256),
        stored_vectors[0].reshape(448, 6, LAYERS, 256),
    )
    return corr.T[None], solver


def solution(mesh):
    in_specs = (
        P("tm", None, None, None, "space", None),
        P("tm", None, None, None, None, "space", None),
        P("tm", None, None, None, "space", None),
    )
    out_specs = (P("tm", "space", None), P("space", None, "tm", None))
    return jax.shard_map(shards, mesh=mesh, in_specs=in_specs, out_specs=out_specs, check_vma=False)
```

```python
import jax
import jax.numpy as jnp
from jax import lax
from jax.experimental import pallas as pl
from jax.experimental.pallas import tpu as pltpu
from jax.sharding import PartitionSpec as P

F32 = jnp.float32
BF16 = jnp.bfloat16

NVEC = 32
LZ = 16
LAYERS = 8
HALVES = 2
LANES = 128
PC = 6
ROWS = 24
FIRST = 8
LAST = 15
BELOW = 7
ABOVE = 16
BATCHES = 8
PER_BATCH = NVEC // BATCHES
HALO_ROWS = PC * PER_BATCH * HALVES
APPLICATIONS = 4
STORE_BLOCK = 32
EARLY_BATCHES = 2
LEADS = (0, 0, 3, 6)
UNROLL = 2


def lane_index():
    return lax.broadcasted_iota(jnp.int32, (LAYERS, LANES), 1)


def y_forward(own, other):
    keep = lane_index() < LANES - LZ
    return jnp.where(keep, pltpu.roll(own, LANES - LZ, 1), pltpu.roll(other, LANES - LZ, 1))


def y_backward(own, other):
    keep = lane_index() >= LZ
    return jnp.where(keep, pltpu.roll(own, LZ, 1), pltpu.roll(other, LZ, 1))


def z_forward(tile):
    along_z = lane_index() % LZ
    return jnp.where(along_z == LZ - 1, pltpu.roll(tile, LZ - 1, 1), pltpu.roll(tile, LANES - 1, 1))


def z_backward(tile):
    along_z = lane_index() % LZ
    return jnp.where(along_z == 0, pltpu.roll(tile, LANES - LZ + 1, 1), pltpu.roll(tile, 1, 1))


def kernel(
    start_ref, links_ref, stored_ref, corr_ref, got_ref,
    x_buf, a_buf, b_buf, raw, coef, edge, top_send, top_recv, halo_send, halo_recv,
    stored, blocks, turned, product, diagonal, ones, delta, part_send, part_recv,
    in_sem, stored_sem, top_sem, halo_send_sem, halo_recv_sem,
    block_send_sem, block_recv_sem, own_sem, part_send_sem, part_recv_sem, met_sem,
):
    me_t = lax.axis_index("tm")
    me_s = lax.axis_index("space")
    up = lax.rem(me_s + 1, 4)
    down = lax.rem(me_s + 3, 4)
    target_space = me_t // 8
    source_first = me_s * 8
    has_self = target_space == me_s

    copies_in = []
    for h in range(HALVES):
        lanes = pl.ds(h * LANES, LANES)
        copies_in.append(pltpu.make_async_copy(
            start_ref.at[:, :, :, :, lanes],
            x_buf.at[:, :, :, h, pl.ds(FIRST, LAYERS), :],
            in_sem.at[h],
        ))
        copies_in.append(pltpu.make_async_copy(
            links_ref.at[:, :, :, :, lanes],
            raw.at[:, :, :, h, pl.ds(FIRST, LAYERS), :],
            in_sem.at[2 + h],
        ))
    for copy in copies_in:
        copy.start()
    stored_copy = pltpu.make_async_copy(stored_ref, stored, stored_sem)
    stored_copy.start()

    y_lo, x_at, z_at = me_t // 16, lax.rem(me_t // 4, 4), lax.rem(me_t, 4)

    def x_partner(step):
        return (y_lo * 16 + lax.rem(x_at + step, 4) * 4 + z_at, me_s)

    def z_partner(step):
        return (y_lo * 16 + x_at * 4 + lax.rem(z_at + step, 4), me_s)

    def y_partner(step):
        return (lax.rem(y_lo + step // 4, 2) * 16 + x_at * 4 + z_at, lax.rem(me_s + step, 4))

    rings = ([x_partner(i) for i in range(1, 4)], [z_partner(i) for i in range(1, 4)], [y_partner(i) for i in range(1, 8)])

    def tell(sem, ring):
        for partner in ring:
            pl.semaphore_signal(sem, inc=1, device_id=partner, device_id_type=pl.DeviceIdType.MESH)

    barrier = pltpu.get_barrier_semaphore()
    for ring in rings:
        tell(barrier, ring)

    def flat(buf):
        return buf.reshape(PC * NVEC * HALVES * ROWS, LANES)

    raw_rows = raw.reshape(54 * HALVES * ROWS, LANES)
    zeros = jnp.zeros((LAYERS, LANES), F32)

    def clear(i, carry):
        for buf in (x_buf, a_buf, b_buf):
            for row in (BELOW, ABOVE):
                flat(buf)[pl.ds(i * LAYERS * ROWS + row, LAYERS, stride=ROWS), :] = zeros
        return carry

    lax.fori_loop(0, PC * NVEC * HALVES // LAYERS, clear, 0)
    group = lax.broadcasted_iota(jnp.int32, (896, LANES), 0) // LAYERS
    ones[...] = jnp.where(group == lax.broadcasted_iota(jnp.int32, (896, LANES), 1), 1.0, 0.0).astype(BF16)
    for i in range(5):
        raw_rows[pl.ds(min(i * LAYERS, 28) * ROWS + BELOW, LAYERS, stride=ROWS), :] = zeros

    copies_in[1].wait()
    copies_in[3].wait()

    top_send[...] = raw_rows[pl.ds(LAST, 36, stride=ROWS), :]

    top_copy = pltpu.make_async_remote_copy(
        top_send, top_recv, top_sem.at[0], top_sem.at[1],
        device_id={"space": up}, device_id_type=pl.DeviceIdType.MESH,
    )

    def halo_copy(level, side, batch):
        return pltpu.make_async_remote_copy(
            halo_send.at[level, side, batch],
            halo_recv.at[level, side, batch],
            halo_send_sem.at[level, side, batch],
            halo_recv_sem.at[level, side, batch],
            device_id={"space": up if side else down},
            device_id_type=pl.DeviceIdType.MESH,
        )

    def send_halo(level, buf, batch):
        rows = flat(buf)
        for side in range(2):
            row = LAST if side else FIRST
            pieces = []
            for pc in range(PC):
                base = ((pc * NVEC + batch * PER_BATCH) * HALVES) * ROWS + row
                pieces.append(rows[pl.ds(base, PER_BATCH * HALVES, stride=ROWS), :])
            halo_send[level, side, batch] = jnp.concatenate(pieces, axis=0).astype(BF16)
            halo_copy(level, side, batch).start()

    def put(direction, entry, half, re, im):
        coef[direction, entry, 0, half] = re
        coef[direction, entry, 1, half] = im - re
        coef[direction, entry, 2, half] = re + im

    def centre(d, part, entry, half):
        return raw[d, part, entry, half, FIRST:FIRST + LAYERS, :]

    def prepare(entry, carry):
        mirrored = lax.rem(entry, 3) * 3 + entry // 3
        for d in range(3):
            for half in range(HALVES):
                put(2 * d, entry, half, centre(d, 0, entry, half), centre(d, 1, entry, half))
        for half in range(HALVES):
            re, im = [y_backward(centre(1, part, entry, half), centre(1, part, entry, 1 - half)) for part in range(2)]
            put(3, mirrored, half, re, -im)
            put(5, mirrored, half, z_backward(centre(2, 0, entry, half)), -z_backward(centre(2, 1, entry, half)))
        return carry

    lax.fori_loop(0, 9, prepare, 0)

    def prepare_below(entry, carry):
        mirrored = lax.rem(entry, 3) * 3 + entry // 3
        for half in range(HALVES):
            re = raw[0, 0, entry, half, pl.ds(BELOW, LAYERS), :]
            im = raw[0, 1, entry, half, pl.ds(BELOW, LAYERS), :]
            put(1, mirrored, half, re, -im)
        return carry

    lax.fori_loop(0, 9, prepare_below, 0)

    edge_rows = coef.reshape(6 * 9 * 3 * HALVES * LAYERS, LANES)
    half_of = lax.broadcasted_iota(jnp.int32, (LAYERS, LANES), 0) % HALVES

    def alternate(rows, first, step):
        low = jnp.broadcast_to(rows[pl.ds(first, 1), :], (LAYERS, LANES))
        high = jnp.broadcast_to(rows[pl.ds(first + step, 1), :], (LAYERS, LANES))
        return jnp.where(half_of == 0, low, high)

    def prepare_above_edge(entry, carry):
        for kind in range(3):
            edge[0, entry, kind] = alternate(edge_rows, (entry * 3 + kind) * HALVES * LAYERS + LAYERS - 1, LAYERS)
        return carry

    lax.fori_loop(0, 9, prepare_above_edge, 0)

    def prepare_below_edge(entry, carry):
        mirrored = lax.rem(entry, 3) * 3 + entry // 3
        re = alternate(top_recv, entry * HALVES, 1)
        im = -alternate(top_recv, (9 + entry) * HALVES, 1)
        edge[1, mirrored, 0] = re
        edge[1, mirrored, 1] = im - re
        edge[1, mirrored, 2] = re + im
        return carry

    def correct(level, buf, batch):
        for side in range(2):
            halo_copy(level, side, batch).wait_recv()
            row = FIRST if side else LAST
            values = halo_recv[level, side, batch].astype(F32)
            count = PER_BATCH * HALVES
            parts = [values[pc * count:(pc + 1) * count] for pc in range(PC)]
            both = [parts[c] + parts[3 + c] for c in range(3)]
            for r in range(3):
                s = [None] * 3
                for c in range(3):
                    for kind, value in enumerate((both[c], parts[c], parts[3 + c])):
                        term = edge[side, r * 3 + c, kind] * value
                        s[kind] = term if s[kind] is None else s[kind] + term
                for pc, change in ((r, s[0] - s[2]), (3 + r, s[0] + s[1])):
                    if level == 3:
                        delta[side, pc, pl.ds(pl.multiple_of(batch * count, count), count), :] = change * (1.0 / 162.0)
                    else:
                        rows = flat(buf)
                        at = pl.ds(((pc * NVEC + batch * PER_BATCH) * HALVES) * ROWS + row, count, stride=ROWS)
                        rows[at, :] = rows[at, :] + change

    def hop_sums(src, vectors, half):
        sums = [[None] * 9 for _ in vectors]

        def add(direction, parts_of):
            for row in range(3):
                for col in range(3):
                    for kind in range(3):
                        factor = coef[direction, row * 3 + col, kind, half]
                        at = row * 3 + kind
                        for i, parts in enumerate(parts_of):
                            term = factor * parts[((6, 0, 3)[kind]) + col]
                            sums[i][at] = term if sums[i][at] is None else sums[i][at] + term

        def extended(parts):
            return parts + [parts[c] + parts[3 + c] for c in range(3)]

        def tiles(v, half_of, first):
            return [src[pc // 3, pc % 3, v, half_of, pl.ds(first, LAYERS), :] for pc in range(PC)]

        own = [tiles(v, half, FIRST) for v in vectors]
        other = [tiles(v, 1 - half, FIRST) for v in vectors]
        add(0, [extended(tiles(v, half, FIRST + 1)) for v in vectors])
        add(1, [extended(tiles(v, half, FIRST - 1)) for v in vectors])
        for direction, shift in ((2, y_forward), (3, y_backward)):
            add(direction, [extended([shift(a, b) for a, b in zip(mine, theirs)]) for mine, theirs in zip(own, other)])
        for direction, shift in ((4, z_forward), (5, z_backward)):
            add(direction, [extended([shift(a) for a in mine]) for mine in own])
        out = []
        for s, mine in zip(sums, own):
            re = [s[3 * r] - s[3 * r + 2] + 0.5 * mine[r] for r in range(3)]
            im = [s[3 * r] + s[3 * r + 1] + 0.5 * mine[3 + r] for r in range(3)]
            out.append(re + im)
        return out

    def apply_pair(level, src, dst, v, half):
        vectors = [v, v + 1]
        for at_v, out in zip(vectors, hop_sums(src, vectors, half)):
            for pc in range(PC):
                value = out[pc]
                at = (pc // 3, pc % 3, at_v, half, pl.ds(FIRST, LAYERS), slice(None))
                if level == 1:
                    value = value - 36.0 * x_buf[at]
                if level == 3:
                    value = value * (1.0 / 162.0) + x_buf[at]
                dst[at] = value

    def correct_source(level, src, batch):
        correct(level - 1, src, batch)
        send_halo(level, src, batch)

    def correct_ahead(level, src, batch):
        ahead = batch + LEADS[level]

        @pl.when(ahead < BATCHES)
        def _():
            correct_source(level, src, ahead)

    def correct_first(level, src):
        def step(batch, carry):
            correct_source(level, src, batch)
            return carry

        lax.fori_loop(0, LEADS[level], step, 0)

    def batches(level, src, dst, first, last):
        def step(batch, carry):
            if level:
                correct_ahead(level, src, batch)

            def pair(i, inner):
                apply_pair(level, src, dst, batch * PER_BATCH + 2 * (i // HALVES), lax.rem(i, HALVES))
                return inner

            lax.fori_loop(0, PER_BATCH, pair, 0, unroll=UNROLL)
            return carry

        lax.fori_loop(first, last, step, 0)

    def first_halo(batch, carry):
        send_halo(0, x_buf, batch)
        return carry

    copies_in[0].wait()
    copies_in[2].wait()
    batches(0, x_buf, a_buf, 0, EARLY_BATCHES)
    pl.semaphore_wait(barrier, sum(len(ring) for ring in rings))
    top_copy.start()
    lax.fori_loop(0, BATCHES, first_halo, 0)
    tell(met_sem.at[0], rings[0])
    batches(0, x_buf, a_buf, EARLY_BATCHES, BATCHES)
    top_copy.wait_recv()
    lax.fori_loop(0, 9, prepare_below_edge, 0)
    pl.semaphore_wait(met_sem.at[0], len(rings[0]))
    tell(met_sem.at[1], rings[1])
    batches(1, a_buf, b_buf, 0, BATCHES)
    pl.semaphore_wait(met_sem.at[1], len(rings[1]))
    tell(met_sem.at[2], rings[2])
    correct_first(2, b_buf)
    batches(2, b_buf, a_buf, 0, BATCHES)
    correct_first(3, a_buf)

    result_rows = flat(b_buf)
    local_t = lax.rem(me_t, 8)

    def block_copy(tm_of):
        return pltpu.make_async_remote_copy(
            blocks.at[tm_of],
            got_ref.at[local_t, me_s],
            block_send_sem.at[tm_of],
            block_recv_sem.at[local_t * 4 + me_s],
            device_id=(tm_of, target_space),
            device_id_type=pl.DeviceIdType.MESH,
        )

    own_copy = pltpu.make_async_copy(blocks.at[me_t], got_ref.at[local_t, me_s], own_sem)

    def destination(half, i):
        return half * 16 + lax.rem(x_at + i // 4, 4) * 4 + lax.rem(z_at + i, 4)

    def foreign(tm_of):
        return jnp.logical_not(jnp.logical_and(has_self, tm_of == me_t))

    def last_half(half):
        def step(batch, carry):
            if half == 0:
                correct_ahead(3, a_buf, batch)

            def pair(i, inner):
                apply_pair(3, a_buf, b_buf, batch * PER_BATCH + 2 * i, half)
                return inner

            lax.fori_loop(0, PER_BATCH // 2, pair, 0, unroll=UNROLL)
            return carry

        lax.fori_loop(0, BATCHES, step, 0)

        if half == 0:
            def last_corrections(batch, carry):
                correct(3, None, batch)
                return carry

            lax.fori_loop(0, BATCHES, last_corrections, 0)

        for side in range(2):
            row = FIRST if side else LAST
            for pc in range(PC):
                at = pl.ds((pc * NVEC * HALVES + half) * ROWS + row, NVEC, stride=HALVES * ROWS)
                result_rows[at, :] = result_rows[at, :] + delta[side, pc, pl.ds(half, NVEC, stride=HALVES), :]

        def arrange(layer, carry):
            tiles = []
            for x in (layer, layer + 4):
                pieces = []
                for pc in range(PC):
                    base = (pc * NVEC * HALVES + half) * ROWS + FIRST + x
                    pieces.append(result_rows[pl.ds(base, NVEC, stride=HALVES * ROWS), :])
                tiles.append(pieces)
                blocks[half * 16:(half + 1) * 16, x] = jnp.concatenate(pieces[:4], axis=0).T.astype(BF16).reshape(16, 8, LANES)
                for c in range(3):
                    re, im = pieces[c].astype(BF16), pieces[3 + c].astype(BF16)
                    at = pl.ds(pl.multiple_of(x * 64, 64), 64)
                    first = c * 256 + half * LANES
                    turned[at, first:first + LANES] = jnp.concatenate([re, im], axis=0)
                    turned[at, 768 + first:768 + first + LANES] = jnp.concatenate([im, -re], axis=0)
            rest = jnp.concatenate(tiles[0][4:] + tiles[1][4:], axis=0)
            blocks[half * 16:(half + 1) * 16, 8 + layer] = rest.T.astype(BF16).reshape(16, 8, LANES)
            return carry

        lax.fori_loop(0, 4, arrange, 0)

        if half == 0:
            pl.semaphore_wait(met_sem.at[2], len(rings[2]))

        def send_block(i, carry):
            tm_of = destination(half, i)

            @pl.when(foreign(tm_of))
            def _():
                block_copy(tm_of).start()

            return carry

        lax.fori_loop(0, 16, send_block, 0)

    last_half(0)
    last_half(1)

    @pl.when(has_self)
    def _():
        own_copy.start()

    stored_copy.wait()

    def correlate(block, carry):
        first = pl.multiple_of(block * STORE_BLOCK, STORE_BLOCK)
        some = [stored[pl.ds(first, STORE_BLOCK), rc].reshape(STORE_BLOCK * LAYERS, 256) for rc in range(PC)]
        product[...] = lax.dot_general(
            turned[...], jnp.concatenate(some, axis=1), (((1,), (1,)), ((), ())), preferred_element_type=F32
        )
        layer = lax.broadcasted_iota(jnp.int32, (64, STORE_BLOCK * LAYERS), 1) % LAYERS
        total = product[0:64]
        for x in range(1, LAYERS):
            total = jnp.where(layer == x, product[x * 64:(x + 1) * 64], total)
        diagonal[:, pl.ds(pl.multiple_of(block * 256, 256), 256)] = total
        return carry

    lax.fori_loop(0, 448 // STORE_BLOCK, correlate, 0)

    def part_copy(step):
        other = lax.rem(me_s + step, 4)
        return pltpu.make_async_remote_copy(
            part_send.at[other],
            part_recv.at[step - 1],
            part_send_sem.at[step - 1],
            part_recv_sem.at[step - 1],
            device_id={"space": other},
            device_id_type=pl.DeviceIdType.MESH,
        )

    for owner in range(4):
        values = diagonal[:, owner * 896:(owner + 1) * 896]
        high = values.astype(BF16)
        low = (values - high.astype(F32)).astype(BF16)
        both = jnp.dot(jnp.concatenate([high, low], axis=0), ones[...], preferred_element_type=F32)
        part_send[owner] = both[:64] + both[64:]
    for step in range(1, 4):
        part_copy(step).start()
    total = part_send[me_s]
    for step in range(1, 4):
        part_copy(step).wait_recv()
        total = total + part_recv[step - 1]
    corr_ref[...] = total[:, :112]

    def finish_halo(i, carry):
        for level in range(APPLICATIONS):
            for side in range(2):
                halo_copy(level, side, i).wait_send()
        return carry

    lax.fori_loop(0, BATCHES, finish_halo, 0)
    top_copy.wait_send()
    for step in range(1, 4):
        part_copy(step).wait_send()

    @pl.when(has_self)
    def _():
        own_copy.wait()

    def finish_block(i, carry):
        for half in range(HALVES):
            tm_of = destination(half, i)

            @pl.when(foreign(tm_of))
            def _():
                block_copy(tm_of).wait_send()

        return carry

    lax.fori_loop(0, 16, finish_block, 0)

    def take_block(i, carry):
        tm_of = source_first + i // 4
        space_of = lax.rem(i, 4)

        @pl.when(jnp.logical_not(jnp.logical_and(tm_of == me_t, space_of == me_s)))
        def _():
            pltpu.make_async_remote_copy(
                blocks.at[0],
                got_ref.at[i // 4, space_of],
                block_send_sem.at[0],
                block_recv_sem.at[i],
                device_id=(tm_of, space_of),
                device_id_type=pl.DeviceIdType.MESH,
            ).wait_recv()

        return carry

    lax.fori_loop(0, 32, take_block, 0)


def unpack(corr_ref, got_ref, corr_out, solver_out):
    corr_out[...] = corr_ref[...]
    for t in range(2):
        for s in range(4):
            solver_out[t, s * 8:(s + 1) * 8, :, :LANES] = got_ref[t, s, 0:8]
            rest = got_ref[t, s, 8:12]
            solver_out[t, s * 8:s * 8 + 4, :, LANES:] = rest[:, :, :64]
            solver_out[t, s * 8 + 4:s * 8 + 8, :, LANES:] = rest[:, :, 64:]


def shards(start_block, gauge_links, stored_vectors):
    any_space = pl.BlockSpec(memory_space=pl.ANY)
    buffer = pltpu.VMEM((2, 3, NVEC, HALVES, ROWS, LANES), F32)
    halo = pltpu.VMEM((APPLICATIONS, 2, BATCHES, HALO_ROWS, LANES), BF16)
    halo_sem = pltpu.SemaphoreType.DMA((APPLICATIONS, 2, BATCHES))
    corr, got = pl.pallas_call(
        kernel,
        out_shape=(
            jax.ShapeDtypeStruct((64, 112), F32),
            jax.ShapeDtypeStruct((8, 4, 12, 8, LANES), BF16),
        ),
        in_specs=[any_space] * 3,
        out_specs=(pl.BlockSpec(memory_space=pltpu.VMEM), any_space),
        scratch_shapes=[
            buffer, buffer, buffer,
            pltpu.VMEM((3, 2, 9, HALVES, ROWS, LANES), F32),
            pltpu.VMEM((6, 9, 3, HALVES, LAYERS, LANES), F32),
            pltpu.VMEM((2, 9, 3, LAYERS, LANES), F32),
            pltpu.VMEM((36, LANES), F32),
            pltpu.VMEM((36, LANES), F32),
            halo, halo,
            pltpu.VMEM((448, 6, LAYERS, 256), BF16),
            pltpu.VMEM((32, 12, 8, LANES), BF16),
            pltpu.VMEM((512, 1536), BF16),
            pltpu.VMEM((512, STORE_BLOCK * LAYERS), F32),
            pltpu.VMEM((64, 448 * LAYERS), F32),
            pltpu.VMEM((896, LANES), BF16),
            pltpu.VMEM((2, PC, NVEC * HALVES, LANES), F32),
            pltpu.VMEM((4, 64, LANES), F32),
            pltpu.VMEM((3, 64, LANES), F32),
            pltpu.SemaphoreType.DMA((4,)),
            pltpu.SemaphoreType.DMA,
            pltpu.SemaphoreType.DMA((2,)),
            halo_sem, halo_sem,
            pltpu.SemaphoreType.DMA((32,)),
            pltpu.SemaphoreType.DMA((32,)),
            pltpu.SemaphoreType.DMA,
            pltpu.SemaphoreType.DMA((3,)),
            pltpu.SemaphoreType.DMA((3,)),
            pltpu.SemaphoreType.REGULAR((3,)),
        ],
        compiler_params=pltpu.CompilerParams(
            collective_id=0, has_side_effects=True, vmem_limit_bytes=60 * 1024 * 1024
        ),
    )(
        start_block[0],
        gauge_links[0].reshape(3, 2, 9, LAYERS, 256),
        stored_vectors[0].reshape(448, 6, LAYERS, 256),
    )
    corr, solver = pl.pallas_call(
        unpack,
        grid=(4,),
        out_shape=(
            jax.ShapeDtypeStruct((64, 112), F32),
            jax.ShapeDtypeStruct((8, 32, 8, 192), BF16),
        ),
        in_specs=[
            pl.BlockSpec((64, 112), lambda i: (0, 0)),
            pl.BlockSpec((2, 4, 12, 8, LANES), lambda i: (i, 0, 0, 0, 0)),
        ],
        out_specs=(
            pl.BlockSpec((64, 112), lambda i: (0, 0)),
            pl.BlockSpec((2, 32, 8, 192), lambda i: (i, 0, 0, 0)),
        ),
    )(corr, got)
    return corr.T[None], solver


def solution(mesh):
    in_specs = (
        P("tm", None, None, None, "space", None),
        P("tm", None, None, None, None, "space", None),
        P("tm", None, None, None, "space", None),
    )
    out_specs = (P("tm", "space", None), P("space", None, "tm", None))
    return jax.shard_map(shards, mesh=mesh, in_specs=in_specs, out_specs=out_specs, check_vma=False)
```

```python
import jax
import jax.numpy as jnp
from jax import lax
from jax.experimental import pallas as pl
from jax.experimental.pallas import tpu as pltpu
from jax.sharding import PartitionSpec as P

F32 = jnp.float32
BF16 = jnp.bfloat16

NVEC = 32
LZ = 16
LAYERS = 8
HALVES = 2
LANES = 128
PC = 6
ROWS = 24
FIRST = 8
LAST = 15
BELOW = 7
ABOVE = 16
BATCHES = 8
PER_BATCH = NVEC // BATCHES
HALO_ROWS = PC * PER_BATCH * HALVES
APPLICATIONS = 4
STORE_BLOCK = 28
EARLY_BATCHES = 2
LEADS = (0, 0, 3, 6)
STEPS = tuple(
    sorted(((dx, dz) for dx in range(4) for dz in range(4)), key=lambda d: (-sum(min(a, 4 - a) for a in d), d))
)


def lane_index():
    return lax.broadcasted_iota(jnp.int32, (LAYERS, LANES), 1)


def y_forward(own, other):
    keep = lane_index() < LANES - LZ
    return jnp.where(keep, pltpu.roll(own, LANES - LZ, 1), pltpu.roll(other, LANES - LZ, 1))


def y_backward(own, other):
    keep = lane_index() >= LZ
    return jnp.where(keep, pltpu.roll(own, LZ, 1), pltpu.roll(other, LZ, 1))


def z_forward(tile):
    along_z = lane_index() % LZ
    return jnp.where(along_z == LZ - 1, pltpu.roll(tile, LZ - 1, 1), pltpu.roll(tile, LANES - 1, 1))


def z_backward(tile):
    along_z = lane_index() % LZ
    return jnp.where(along_z == 0, pltpu.roll(tile, LANES - LZ + 1, 1), pltpu.roll(tile, 1, 1))


def kernel(
    start_ref, links_ref, stored_ref, corr_ref, got_ref,
    x_buf, a_buf, b_buf, raw, coef, edge, top_send, top_recv, halo_send, halo_recv,
    stored, blocks, turned, product, diagonal, ones, delta, part_send, part_recv,
    in_sem, stored_sem, top_sem, halo_send_sem, halo_recv_sem,
    block_send_sem, block_recv_sem, own_sem, part_send_sem, part_recv_sem, met_sem,
):
    me_t = lax.axis_index("tm")
    me_s = lax.axis_index("space")
    up = lax.rem(me_s + 1, 4)
    down = lax.rem(me_s + 3, 4)
    target_space = me_t // 8
    source_first = me_s * 8
    has_self = target_space == me_s

    copies_in = []
    for h in range(HALVES):
        lanes = pl.ds(h * LANES, LANES)
        copies_in.append(pltpu.make_async_copy(
            start_ref.at[:, :, :, :, lanes],
            x_buf.at[:, :, :, h, pl.ds(FIRST, LAYERS), :],
            in_sem.at[h],
        ))
        copies_in.append(pltpu.make_async_copy(
            links_ref.at[:, :, :, :, lanes],
            raw.at[:, :, :, h, pl.ds(FIRST, LAYERS), :],
            in_sem.at[2 + h],
        ))
    for copy in copies_in:
        copy.start()
    stored_copy = pltpu.make_async_copy(stored_ref, stored, stored_sem)
    stored_copy.start()

    y_lo, x_at, z_at = me_t // 16, lax.rem(me_t // 4, 4), lax.rem(me_t, 4)

    def x_partner(step):
        return (y_lo * 16 + lax.rem(x_at + step, 4) * 4 + z_at, me_s)

    def z_partner(step):
        return (y_lo * 16 + x_at * 4 + lax.rem(z_at + step, 4), me_s)

    def y_partner(step):
        return (lax.rem(y_lo + step // 4, 2) * 16 + x_at * 4 + z_at, lax.rem(me_s + step, 4))

    rings = ([x_partner(i) for i in range(1, 4)], [z_partner(i) for i in range(1, 4)], [y_partner(i) for i in range(1, 8)])

    def tell(sem, ring):
        for partner in ring:
            pl.semaphore_signal(sem, inc=1, device_id=partner, device_id_type=pl.DeviceIdType.MESH)

    barrier = pltpu.get_barrier_semaphore()
    for ring in rings:
        tell(barrier, ring)

    def flat(buf):
        return buf.reshape(PC * NVEC * HALVES * ROWS, LANES)

    raw_rows = raw.reshape(54 * HALVES * ROWS, LANES)
    zeros = jnp.zeros((LAYERS, LANES), F32)

    def clear(i, carry):
        for buf in (x_buf, a_buf, b_buf):
            for row in (BELOW, ABOVE):
                flat(buf)[pl.ds(i * LAYERS * ROWS + row, LAYERS, stride=ROWS), :] = zeros
        return carry

    lax.fori_loop(0, PC * NVEC * HALVES // LAYERS, clear, 0)
    column = lax.broadcasted_iota(jnp.int32, (1024, LANES), 0)
    group = jnp.where(column % 256 < STORE_BLOCK * LAYERS, column // 256 * STORE_BLOCK + column % 256 // LAYERS, -1)
    ones[...] = jnp.where(group == lax.broadcasted_iota(jnp.int32, (1024, LANES), 1), 1.0, 0.0).astype(BF16)
    diagonal[...] = jnp.zeros_like(diagonal)
    for i in range(5):
        raw_rows[pl.ds(min(i * LAYERS, 28) * ROWS + BELOW, LAYERS, stride=ROWS), :] = zeros

    copies_in[1].wait()
    copies_in[3].wait()

    top_send[...] = raw_rows[pl.ds(LAST, 36, stride=ROWS), :]

    top_copy = pltpu.make_async_remote_copy(
        top_send, top_recv, top_sem.at[0], top_sem.at[1],
        device_id={"space": up}, device_id_type=pl.DeviceIdType.MESH,
    )

    def halo_copy(level, side, batch):
        return pltpu.make_async_remote_copy(
            halo_send.at[level, side, batch],
            halo_recv.at[level, side, batch],
            halo_send_sem.at[level, side, batch],
            halo_recv_sem.at[level, side, batch],
            device_id={"space": up if side else down},
            device_id_type=pl.DeviceIdType.MESH,
        )

    def send_halo(level, buf, batch):
        rows = flat(buf)
        for side in range(2):
            row = LAST if side else FIRST
            pieces = []
            for pc in range(PC):
                base = ((pc * NVEC + batch * PER_BATCH) * HALVES) * ROWS + row
                pieces.append(rows[pl.ds(base, PER_BATCH * HALVES, stride=ROWS), :])
            halo_send[level, side, batch] = jnp.concatenate(pieces, axis=0).astype(BF16)
            halo_copy(level, side, batch).start()

    def put(direction, entry, half, re, im):
        coef[direction, entry, 0, half] = re
        coef[direction, entry, 1, half] = im - re
        coef[direction, entry, 2, half] = re + im

    def centre(d, part, entry, half):
        return raw[d, part, entry, half, FIRST:FIRST + LAYERS, :]

    def prepare(entry, carry):
        mirrored = lax.rem(entry, 3) * 3 + entry // 3
        for d in range(3):
            for half in range(HALVES):
                put(2 * d, entry, half, centre(d, 0, entry, half), centre(d, 1, entry, half))
        for half in range(HALVES):
            re, im = [y_backward(centre(1, part, entry, half), centre(1, part, entry, 1 - half)) for part in range(2)]
            put(3, mirrored, half, re, -im)
            put(5, mirrored, half, z_backward(centre(2, 0, entry, half)), -z_backward(centre(2, 1, entry, half)))
        return carry

    lax.fori_loop(0, 9, prepare, 0)

    def prepare_below(entry, carry):
        mirrored = lax.rem(entry, 3) * 3 + entry // 3
        for half in range(HALVES):
            re = raw[0, 0, entry, half, pl.ds(BELOW, LAYERS), :]
            im = raw[0, 1, entry, half, pl.ds(BELOW, LAYERS), :]
            put(1, mirrored, half, re, -im)
        return carry

    lax.fori_loop(0, 9, prepare_below, 0)

    edge_rows = coef.reshape(6 * 9 * 3 * HALVES * LAYERS, LANES)
    half_of = lax.broadcasted_iota(jnp.int32, (LAYERS, LANES), 0) % HALVES

    def alternate(rows, first, step):
        low = jnp.broadcast_to(rows[pl.ds(first, 1), :], (LAYERS, LANES))
        high = jnp.broadcast_to(rows[pl.ds(first + step, 1), :], (LAYERS, LANES))
        return jnp.where(half_of == 0, low, high)

    def prepare_above_edge(entry, carry):
        for kind in range(3):
            edge[0, entry, kind] = alternate(edge_rows, (entry * 3 + kind) * HALVES * LAYERS + LAYERS - 1, LAYERS)
        return carry

    lax.fori_loop(0, 9, prepare_above_edge, 0)

    def prepare_below_edge(entry, carry):
        mirrored = lax.rem(entry, 3) * 3 + entry // 3
        re = alternate(top_recv, entry * HALVES, 1)
        im = -alternate(top_recv, (9 + entry) * HALVES, 1)
        edge[1, mirrored, 0] = re
        edge[1, mirrored, 1] = im - re
        edge[1, mirrored, 2] = re + im
        return carry

    def correct(level, buf, batch):
        for side in range(2):
            halo_copy(level, side, batch).wait_recv()
            row = FIRST if side else LAST
            values = halo_recv[level, side, batch].astype(F32)
            count = PER_BATCH * HALVES
            parts = [values[pc * count:(pc + 1) * count] for pc in range(PC)]
            both = [parts[c] + parts[3 + c] for c in range(3)]
            for r in range(3):
                s = [None] * 3
                for c in range(3):
                    for kind, value in enumerate((both[c], parts[c], parts[3 + c])):
                        term = edge[side, r * 3 + c, kind] * value
                        s[kind] = term if s[kind] is None else s[kind] + term
                for pc, change in ((r, s[0] - s[2]), (3 + r, s[0] + s[1])):
                    if level == 3:
                        delta[side, pc, pl.ds(pl.multiple_of(batch * count, count), count), :] = change * (1.0 / 162.0)
                    else:
                        rows = flat(buf)
                        at = pl.ds(((pc * NVEC + batch * PER_BATCH) * HALVES) * ROWS + row, count, stride=ROWS)
                        rows[at, :] = rows[at, :] + change

    def hop_sums(src, vectors, half):
        sums = [[None] * 9 for _ in vectors]

        def add(direction, parts_of):
            for row in range(3):
                for col in range(3):
                    for kind in range(3):
                        factor = coef[direction, row * 3 + col, kind, half]
                        at = row * 3 + kind
                        for i, parts in enumerate(parts_of):
                            term = factor * parts[((6, 0, 3)[kind]) + col]
                            sums[i][at] = term if sums[i][at] is None else sums[i][at] + term

        def extended(parts):
            return parts + [parts[c] + parts[3 + c] for c in range(3)]

        def tiles(v, half_of, first):
            return [src[pc // 3, pc % 3, v, half_of, pl.ds(first, LAYERS), :] for pc in range(PC)]

        own = [tiles(v, half, FIRST) for v in vectors]
        other = [tiles(v, 1 - half, FIRST) for v in vectors]
        add(0, [extended(tiles(v, half, FIRST + 1)) for v in vectors])
        add(1, [extended(tiles(v, half, FIRST - 1)) for v in vectors])
        for direction, shift in ((2, y_forward), (3, y_backward)):
            add(direction, [extended([shift(a, b) for a, b in zip(mine, theirs)]) for mine, theirs in zip(own, other)])
        for direction, shift in ((4, z_forward), (5, z_backward)):
            add(direction, [extended([shift(a) for a in mine]) for mine in own])
        out = []
        for s, mine in zip(sums, own):
            re = [s[3 * r] - s[3 * r + 2] + 0.5 * mine[r] for r in range(3)]
            im = [s[3 * r] + s[3 * r + 1] + 0.5 * mine[3 + r] for r in range(3)]
            out.append(re + im)
        return out

    def apply_pair(level, src, dst, v, half):
        vectors = [v, v + 1]
        for at_v, out in zip(vectors, hop_sums(src, vectors, half)):
            for pc in range(PC):
                value = out[pc]
                at = (pc // 3, pc % 3, at_v, half, pl.ds(FIRST, LAYERS), slice(None))
                if level == 1:
                    value = value - 36.0 * x_buf[at]
                if level == 3:
                    value = value * (1.0 / 162.0) + x_buf[at]
                dst[at] = value

    def correct_source(level, src, batch):
        correct(level - 1, src, batch)
        send_halo(level, src, batch)

    def correct_ahead(level, src, batch):
        ahead = batch + LEADS[level]

        @pl.when(ahead < BATCHES)
        def _():
            correct_source(level, src, ahead)

    def correct_first(level, src):
        def step(batch, carry):
            correct_source(level, src, batch)
            return carry

        lax.fori_loop(0, LEADS[level], step, 0)

    def batches(level, src, dst, first, last):
        def step(batch, carry):
            if level:
                correct_ahead(level, src, batch)

            def pair(i, inner):
                apply_pair(level, src, dst, batch * PER_BATCH + 2 * (i // HALVES), lax.rem(i, HALVES))
                return inner

            lax.fori_loop(0, PER_BATCH, pair, 0, unroll=PER_BATCH)
            return carry

        lax.fori_loop(first, last, step, 0)

    def first_halo(batch, carry):
        send_halo(0, x_buf, batch)
        return carry

    copies_in[0].wait()
    copies_in[2].wait()
    batches(0, x_buf, a_buf, 0, EARLY_BATCHES)
    pl.semaphore_wait(barrier, sum(len(ring) for ring in rings))
    top_copy.start()
    lax.fori_loop(0, BATCHES, first_halo, 0)
    tell(met_sem.at[0], rings[0])
    batches(0, x_buf, a_buf, EARLY_BATCHES, BATCHES)
    top_copy.wait_recv()
    lax.fori_loop(0, 9, prepare_below_edge, 0)
    pl.semaphore_wait(met_sem.at[0], len(rings[0]))
    tell(met_sem.at[1], rings[1])
    batches(1, a_buf, b_buf, 0, BATCHES)
    pl.semaphore_wait(met_sem.at[1], len(rings[1]))
    tell(met_sem.at[2], rings[2])
    correct_first(2, b_buf)
    batches(2, b_buf, a_buf, 0, BATCHES)
    correct_first(3, a_buf)

    result_rows = flat(b_buf)
    local_t = lax.rem(me_t, 8)

    def block_copy(tm_of):
        return pltpu.make_async_remote_copy(
            blocks.at[tm_of],
            got_ref.at[local_t, me_s],
            block_send_sem.at[tm_of],
            block_recv_sem.at[local_t * 4 + me_s],
            device_id=(tm_of, target_space),
            device_id_type=pl.DeviceIdType.MESH,
        )

    own_copy = pltpu.make_async_copy(blocks.at[me_t], got_ref.at[local_t, me_s], own_sem)

    def destination(half, i):
        dx, dz = STEPS[i]
        return half * 16 + lax.rem(x_at + dx, 4) * 4 + lax.rem(z_at + dz, 4)

    def foreign(tm_of):
        return jnp.logical_not(jnp.logical_and(has_self, tm_of == me_t))

    def send_block(tm_of):
        @pl.when(foreign(tm_of))
        def _():
            block_copy(tm_of).start()

    def last_half(half):
        def step(batch, carry):
            if half == 0:
                correct_ahead(3, a_buf, batch)

            def pair(i, inner):
                apply_pair(3, a_buf, b_buf, batch * PER_BATCH + 2 * i, half)
                return inner

            lax.fori_loop(0, PER_BATCH // 2, pair, 0, unroll=PER_BATCH // 2)
            return carry

        lax.fori_loop(0, BATCHES, step, 0)

        if half == 0:
            def last_corrections(batch, carry):
                correct(3, None, batch)
                return carry

            lax.fori_loop(0, BATCHES, last_corrections, 0)

        for side in range(2):
            row = FIRST if side else LAST
            for pc in range(PC):
                at = pl.ds((pc * NVEC * HALVES + half) * ROWS + row, NVEC, stride=HALVES * ROWS)
                result_rows[at, :] = result_rows[at, :] + delta[side, pc, pl.ds(half, NVEC, stride=HALVES), :]

        def arrange(layer, carry):
            tiles = []
            for x in (layer, layer + 4):
                pieces = []
                for pc in range(PC):
                    base = (pc * NVEC * HALVES + half) * ROWS + FIRST + x
                    pieces.append(result_rows[pl.ds(base, NVEC, stride=HALVES * ROWS), :])
                tiles.append(pieces)
                blocks[half * 16:(half + 1) * 16, x] = jnp.concatenate(pieces[:4], axis=0).T.astype(BF16).reshape(16, 8, LANES)
                for c in range(3):
                    re, im = pieces[c].astype(BF16), pieces[3 + c].astype(BF16)
                    at = pl.ds(pl.multiple_of(x * 64, 64), 64)
                    first = c * 256 + half * LANES
                    turned[at, first:first + LANES] = jnp.concatenate([re, im], axis=0)
                    turned[at, 768 + first:768 + first + LANES] = jnp.concatenate([im, -re], axis=0)
            rest = jnp.concatenate(tiles[0][4:] + tiles[1][4:], axis=0)
            blocks[half * 16:(half + 1) * 16, 8 + layer] = rest.T.astype(BF16).reshape(16, 8, LANES)
            return carry

        lax.fori_loop(0, 4, arrange, 0)

        if half == 0:
            pl.semaphore_wait(met_sem.at[2], len(rings[2]))

        for i in range(16):
            send_block(destination(half, i))

    last_half(0)
    last_half(1)

    @pl.when(has_self)
    def _():
        own_copy.start()

    stored_copy.wait()

    def part_copy(step):
        other = lax.rem(me_s + step, 4)
        return pltpu.make_async_remote_copy(
            part_send.at[step - 1],
            part_recv.at[step - 1],
            part_send_sem.at[step - 1],
            part_recv_sem.at[step - 1],
            device_id={"space": other},
            device_id_type=pl.DeviceIdType.MESH,
        )

    def correlate(owner):
        def block(j, carry):
            first = owner * 112 + j * STORE_BLOCK
            some = [stored[pl.ds(first, STORE_BLOCK), rc].reshape(STORE_BLOCK * LAYERS, 256) for rc in range(PC)]
            product[...] = lax.dot_general(
                turned[...], jnp.concatenate(some, axis=1), (((1,), (1,)), ((), ())), preferred_element_type=F32
            )
            layer = lax.broadcasted_iota(jnp.int32, (64, STORE_BLOCK * LAYERS), 1) % LAYERS
            total = product[0:64]
            for x in range(1, LAYERS):
                total = jnp.where(layer == x, product[x * 64:(x + 1) * 64], total)
            diagonal[j, :, :STORE_BLOCK * LAYERS] = total
            return carry

        lax.fori_loop(0, 4, block, 0)
        values = jnp.concatenate([diagonal[j] for j in range(4)], axis=1)
        high = values.astype(BF16)
        low = (values - high.astype(F32)).astype(BF16)
        both = jnp.dot(jnp.concatenate([high, low], axis=0), ones[...], preferred_element_type=F32)
        return both[:64] + both[64:]

    def give(step, carry):
        part_send[step - 1] = correlate(lax.rem(me_s + step, 4))
        part_copy(step).start()
        return carry

    lax.fori_loop(1, 4, give, 0)
    total = correlate(me_s)
    for step in range(1, 4):
        part_copy(step).wait_recv()
        total = total + part_recv[step - 1]
    corr_ref[...] = total[:, :112]

    def finish_halo(i, carry):
        for level in range(APPLICATIONS):
            for side in range(2):
                halo_copy(level, side, i).wait_send()
        return carry

    lax.fori_loop(0, BATCHES, finish_halo, 0)
    top_copy.wait_send()
    for step in range(1, 4):
        part_copy(step).wait_send()

    @pl.when(has_self)
    def _():
        own_copy.wait()

    def finish_block(tm_of):
        @pl.when(foreign(tm_of))
        def _():
            block_copy(tm_of).wait_send()

    for half in range(HALVES):
        for i in range(16):
            finish_block(destination(half, i))

    def take_block(i, carry):
        tm_of = source_first + i // 4
        space_of = lax.rem(i, 4)

        @pl.when(jnp.logical_not(jnp.logical_and(tm_of == me_t, space_of == me_s)))
        def _():
            pltpu.make_async_remote_copy(
                blocks.at[0],
                got_ref.at[i // 4, space_of],
                block_send_sem.at[0],
                block_recv_sem.at[i],
                device_id=(tm_of, space_of),
                device_id_type=pl.DeviceIdType.MESH,
            ).wait_recv()

        return carry

    lax.fori_loop(0, 32, take_block, 0)


def unpack(corr_ref, got_ref, corr_out, solver_out):
    corr_out[...] = corr_ref[...]
    for t in range(4):
        for s in range(4):
            solver_out[t, s * 8:(s + 1) * 8, :, :LANES] = got_ref[t, s, 0:8]
            rest = got_ref[t, s, 8:12]
            solver_out[t, s * 8:s * 8 + 4, :, LANES:] = rest[:, :, :64]
            solver_out[t, s * 8 + 4:s * 8 + 8, :, LANES:] = rest[:, :, 64:]


def shards(start_block, gauge_links, stored_vectors):
    any_space = pl.BlockSpec(memory_space=pl.ANY)
    buffer = pltpu.VMEM((2, 3, NVEC, HALVES, ROWS, LANES), F32)
    halo = pltpu.VMEM((APPLICATIONS, 2, BATCHES, HALO_ROWS, LANES), BF16)
    halo_sem = pltpu.SemaphoreType.DMA((APPLICATIONS, 2, BATCHES))
    corr, got = pl.pallas_call(
        kernel,
        out_shape=(
            jax.ShapeDtypeStruct((64, 112), F32),
            jax.ShapeDtypeStruct((8, 4, 12, 8, LANES), BF16),
        ),
        in_specs=[any_space] * 3,
        out_specs=(pl.BlockSpec(memory_space=pltpu.VMEM), any_space),
        scratch_shapes=[
            buffer, buffer, buffer,
            pltpu.VMEM((3, 2, 9, HALVES, ROWS, LANES), F32),
            pltpu.VMEM((6, 9, 3, HALVES, LAYERS, LANES), F32),
            pltpu.VMEM((2, 9, 3, LAYERS, LANES), F32),
            pltpu.VMEM((36, LANES), F32),
            pltpu.VMEM((36, LANES), F32),
            halo, halo,
            pltpu.VMEM((448, 6, LAYERS, 256), BF16),
            pltpu.VMEM((32, 12, 8, LANES), BF16),
            pltpu.VMEM((512, 1536), BF16),
            pltpu.VMEM((512, STORE_BLOCK * LAYERS), F32),
            pltpu.VMEM((4, 64, 256), F32),
            pltpu.VMEM((1024, LANES), BF16),
            pltpu.VMEM((2, PC, NVEC * HALVES, LANES), F32),
            pltpu.VMEM((3, 64, LANES), F32),
            pltpu.VMEM((3, 64, LANES), F32),
            pltpu.SemaphoreType.DMA((4,)),
            pltpu.SemaphoreType.DMA,
            pltpu.SemaphoreType.DMA((2,)),
            halo_sem, halo_sem,
            pltpu.SemaphoreType.DMA((32,)),
            pltpu.SemaphoreType.DMA((32,)),
            pltpu.SemaphoreType.DMA,
            pltpu.SemaphoreType.DMA((3,)),
            pltpu.SemaphoreType.DMA((3,)),
            pltpu.SemaphoreType.REGULAR((3,)),
        ],
        compiler_params=pltpu.CompilerParams(
            collective_id=0, has_side_effects=True, vmem_limit_bytes=60 * 1024 * 1024
        ),
    )(
        start_block[0],
        gauge_links[0].reshape(3, 2, 9, LAYERS, 256),
        stored_vectors[0].reshape(448, 6, LAYERS, 256),
    )
    corr, solver = pl.pallas_call(
        unpack,
        grid=(2,),
        out_shape=(
            jax.ShapeDtypeStruct((64, 112), F32),
            jax.ShapeDtypeStruct((8, 32, 8, 192), BF16),
        ),
        in_specs=[
            pl.BlockSpec((64, 112), lambda i: (0, 0)),
            pl.BlockSpec((4, 4, 12, 8, LANES), lambda i: (i, 0, 0, 0, 0)),
        ],
        out_specs=(
            pl.BlockSpec((64, 112), lambda i: (0, 0)),
            pl.BlockSpec((4, 32, 8, 192), lambda i: (i, 0, 0, 0)),
        ),
    )(corr, got)
    return corr.T[None], solver


def solution(mesh):
    in_specs = (
        P("tm", None, None, None, "space", None),
        P("tm", None, None, None, None, "space", None),
        P("tm", None, None, None, "space", None),
    )
    out_specs = (P("tm", "space", None), P("space", None, "tm", None))
    return jax.shard_map(shards, mesh=mesh, in_specs=in_specs, out_specs=out_specs, check_vma=False)
```

```python
import jax
import jax.numpy as jnp
from jax import lax
from jax.experimental import pallas as pl
from jax.experimental.pallas import tpu as pltpu
from jax.sharding import PartitionSpec as P

F32 = jnp.float32
BF16 = jnp.bfloat16

NVEC = 32
LZ = 16
LAYERS = 8
HALVES = 2
LANES = 128
PC = 6
ROWS = 24
FIRST = 8
LAST = 15
BELOW = 7
ABOVE = 16
BATCHES = 8
PER_BATCH = NVEC // BATCHES
HALO_ROWS = PC * PER_BATCH * HALVES
APPLICATIONS = 4
STORE_BLOCK = 28
EARLY_BATCHES = 2
LEADS = (0, 0, 4, 8)
BEFORE_RELEASE = 2
STEPS = tuple(
    sorted(((dx, dz) for dx in range(4) for dz in range(4)), key=lambda d: (-sum(min(a, 4 - a) for a in d), d))
)


def lane_index():
    return lax.broadcasted_iota(jnp.int32, (LAYERS, LANES), 1)


def y_forward(own, other):
    keep = lane_index() < LANES - LZ
    return jnp.where(keep, pltpu.roll(own, LANES - LZ, 1), pltpu.roll(other, LANES - LZ, 1))


def y_backward(own, other):
    keep = lane_index() >= LZ
    return jnp.where(keep, pltpu.roll(own, LZ, 1), pltpu.roll(other, LZ, 1))


def z_forward(tile):
    along_z = lane_index() % LZ
    return jnp.where(along_z == LZ - 1, pltpu.roll(tile, LZ - 1, 1), pltpu.roll(tile, LANES - 1, 1))


def z_backward(tile):
    along_z = lane_index() % LZ
    return jnp.where(along_z == 0, pltpu.roll(tile, LANES - LZ + 1, 1), pltpu.roll(tile, 1, 1))


def kernel(
    start_ref, links_ref, stored_ref, corr_ref, got_ref,
    x_buf, a_buf, b_buf, raw, coef, edge, top_send, top_recv, halo_send, halo_recv,
    stored, blocks, turned, product, diagonal, ones, delta, part_send, part_recv,
    in_sem, stored_sem, top_sem, halo_send_sem, halo_recv_sem,
    block_send_sem, block_recv_sem, own_sem, part_send_sem, part_recv_sem, met_sem,
):
    me_t = lax.axis_index("tm")
    me_s = lax.axis_index("space")
    up = lax.rem(me_s + 1, 4)
    down = lax.rem(me_s + 3, 4)
    target_space = me_t // 8
    source_first = me_s * 8
    has_self = target_space == me_s

    copies_in = []
    for h in range(HALVES):
        lanes = pl.ds(h * LANES, LANES)
        copies_in.append(pltpu.make_async_copy(
            start_ref.at[:, :, :, :, lanes],
            x_buf.at[:, :, :, h, pl.ds(FIRST, LAYERS), :],
            in_sem.at[h],
        ))
        copies_in.append(pltpu.make_async_copy(
            links_ref.at[:, :, :, :, lanes],
            raw.at[:, :, :, h, pl.ds(FIRST, LAYERS), :],
            in_sem.at[2 + h],
        ))
    for copy in copies_in:
        copy.start()
    stored_copy = pltpu.make_async_copy(stored_ref, stored, stored_sem)
    stored_copy.start()

    y_lo, x_at, z_at = me_t // 16, lax.rem(me_t // 4, 4), lax.rem(me_t, 4)

    def x_partner(step):
        return (y_lo * 16 + lax.rem(x_at + step, 4) * 4 + z_at, me_s)

    def z_partner(step):
        return (y_lo * 16 + x_at * 4 + lax.rem(z_at + step, 4), me_s)

    def y_partner(step):
        return (lax.rem(y_lo + step // 4, 2) * 16 + x_at * 4 + z_at, lax.rem(me_s + step, 4))

    rings = ([x_partner(i) for i in range(1, 4)], [z_partner(i) for i in range(1, 4)], [y_partner(i) for i in range(1, 8)])

    def tell(sem, ring):
        for partner in ring:
            pl.semaphore_signal(sem, inc=1, device_id=partner, device_id_type=pl.DeviceIdType.MESH)

    barrier = pltpu.get_barrier_semaphore()
    for ring in rings:
        tell(barrier, ring)

    def flat(buf):
        return buf.reshape(PC * NVEC * HALVES * ROWS, LANES)

    raw_rows = raw.reshape(54 * HALVES * ROWS, LANES)
    zeros = jnp.zeros((LAYERS, LANES), F32)

    def clear(i, carry):
        for buf in (x_buf, a_buf, b_buf):
            for row in (BELOW, ABOVE):
                flat(buf)[pl.ds(i * LAYERS * ROWS + row, LAYERS, stride=ROWS), :] = zeros
        return carry

    lax.fori_loop(0, PC * NVEC * HALVES // LAYERS, clear, 0)
    column = lax.broadcasted_iota(jnp.int32, (1024, LANES), 0)
    group = jnp.where(column % 256 < STORE_BLOCK * LAYERS, column // 256 * STORE_BLOCK + column % 256 // LAYERS, -1)
    ones[...] = jnp.where(group == lax.broadcasted_iota(jnp.int32, (1024, LANES), 1), 1.0, 0.0).astype(BF16)
    diagonal[...] = jnp.zeros_like(diagonal)
    for i in range(5):
        raw_rows[pl.ds(min(i * LAYERS, 28) * ROWS + BELOW, LAYERS, stride=ROWS), :] = zeros

    copies_in[1].wait()
    copies_in[3].wait()

    top_send[...] = raw_rows[pl.ds(LAST, 36, stride=ROWS), :]

    top_copy = pltpu.make_async_remote_copy(
        top_send, top_recv, top_sem.at[0], top_sem.at[1],
        device_id={"space": up}, device_id_type=pl.DeviceIdType.MESH,
    )

    def halo_copy(level, side, batch):
        return pltpu.make_async_remote_copy(
            halo_send.at[level, side, batch],
            halo_recv.at[level, side, batch],
            halo_send_sem.at[level, side, batch],
            halo_recv_sem.at[level, side, batch],
            device_id={"space": up if side else down},
            device_id_type=pl.DeviceIdType.MESH,
        )

    def send_halo(level, buf, batch):
        rows = flat(buf)
        for side in range(2):
            row = LAST if side else FIRST
            pieces = []
            for pc in range(PC):
                base = ((pc * NVEC + batch * PER_BATCH) * HALVES) * ROWS + row
                pieces.append(rows[pl.ds(base, PER_BATCH * HALVES, stride=ROWS), :])
            halo_send[level, side, batch] = jnp.concatenate(pieces, axis=0).astype(BF16)
            halo_copy(level, side, batch).start()

    def put(direction, entry, half, re, im):
        coef[direction, entry, 0, half] = re
        coef[direction, entry, 1, half] = im - re
        coef[direction, entry, 2, half] = re + im

    def centre(d, part, entry, half):
        return raw[d, part, entry, half, FIRST:FIRST + LAYERS, :]

    def prepare(entry, carry):
        mirrored = lax.rem(entry, 3) * 3 + entry // 3
        for d in range(3):
            for half in range(HALVES):
                put(2 * d, entry, half, centre(d, 0, entry, half), centre(d, 1, entry, half))
        for half in range(HALVES):
            re, im = [y_backward(centre(1, part, entry, half), centre(1, part, entry, 1 - half)) for part in range(2)]
            put(3, mirrored, half, re, -im)
            put(5, mirrored, half, z_backward(centre(2, 0, entry, half)), -z_backward(centre(2, 1, entry, half)))
        return carry

    lax.fori_loop(0, 9, prepare, 0)

    def prepare_below(entry, carry):
        mirrored = lax.rem(entry, 3) * 3 + entry // 3
        for half in range(HALVES):
            re = raw[0, 0, entry, half, pl.ds(BELOW, LAYERS), :]
            im = raw[0, 1, entry, half, pl.ds(BELOW, LAYERS), :]
            put(1, mirrored, half, re, -im)
        return carry

    lax.fori_loop(0, 9, prepare_below, 0)

    edge_rows = coef.reshape(6 * 9 * 3 * HALVES * LAYERS, LANES)
    half_of = lax.broadcasted_iota(jnp.int32, (LAYERS, LANES), 0) % HALVES

    def alternate(rows, first, step):
        low = jnp.broadcast_to(rows[pl.ds(first, 1), :], (LAYERS, LANES))
        high = jnp.broadcast_to(rows[pl.ds(first + step, 1), :], (LAYERS, LANES))
        return jnp.where(half_of == 0, low, high)

    def prepare_above_edge(entry, carry):
        for kind in range(3):
            edge[0, entry, kind] = alternate(edge_rows, (entry * 3 + kind) * HALVES * LAYERS + LAYERS - 1, LAYERS)
        return carry

    lax.fori_loop(0, 9, prepare_above_edge, 0)

    def prepare_below_edge(entry, carry):
        mirrored = lax.rem(entry, 3) * 3 + entry // 3
        re = alternate(top_recv, entry * HALVES, 1)
        im = -alternate(top_recv, (9 + entry) * HALVES, 1)
        edge[1, mirrored, 0] = re
        edge[1, mirrored, 1] = im - re
        edge[1, mirrored, 2] = re + im
        return carry

    def correct(level, buf, batch):
        for side in range(2):
            halo_copy(level, side, batch).wait_recv()
            row = FIRST if side else LAST
            values = halo_recv[level, side, batch].astype(F32)
            count = PER_BATCH * HALVES
            parts = [values[pc * count:(pc + 1) * count] for pc in range(PC)]
            both = [parts[c] + parts[3 + c] for c in range(3)]
            for r in range(3):
                s = [None] * 3
                for c in range(3):
                    for kind, value in enumerate((both[c], parts[c], parts[3 + c])):
                        term = edge[side, r * 3 + c, kind] * value
                        s[kind] = term if s[kind] is None else s[kind] + term
                for pc, change in ((r, s[0] - s[2]), (3 + r, s[0] + s[1])):
                    if level == 3:
                        delta[side, pc, pl.ds(pl.multiple_of(batch * count, count), count), :] = change * (1.0 / 162.0)
                    else:
                        rows = flat(buf)
                        at = pl.ds(((pc * NVEC + batch * PER_BATCH) * HALVES) * ROWS + row, count, stride=ROWS)
                        rows[at, :] = rows[at, :] + change

    def hop_sums(src, vectors, half):
        sums = [[None] * 9 for _ in vectors]

        def add(direction, parts_of):
            for row in range(3):
                for col in range(3):
                    for kind in range(3):
                        factor = coef[direction, row * 3 + col, kind, half]
                        at = row * 3 + kind
                        for i, parts in enumerate(parts_of):
                            term = factor * parts[((6, 0, 3)[kind]) + col]
                            sums[i][at] = term if sums[i][at] is None else sums[i][at] + term

        def extended(parts):
            return parts + [parts[c] + parts[3 + c] for c in range(3)]

        def tiles(v, half_of, first):
            return [src[pc // 3, pc % 3, v, half_of, pl.ds(first, LAYERS), :] for pc in range(PC)]

        own = [tiles(v, half, FIRST) for v in vectors]
        other = [tiles(v, 1 - half, FIRST) for v in vectors]
        add(0, [extended(tiles(v, half, FIRST + 1)) for v in vectors])
        add(1, [extended(tiles(v, half, FIRST - 1)) for v in vectors])
        for direction, shift in ((2, y_forward), (3, y_backward)):
            add(direction, [extended([shift(a, b) for a, b in zip(mine, theirs)]) for mine, theirs in zip(own, other)])
        for direction, shift in ((4, z_forward), (5, z_backward)):
            add(direction, [extended([shift(a) for a in mine]) for mine in own])
        out = []
        for s, mine in zip(sums, own):
            re = [s[3 * r] - s[3 * r + 2] + 0.5 * mine[r] for r in range(3)]
            im = [s[3 * r] + s[3 * r + 1] + 0.5 * mine[3 + r] for r in range(3)]
            out.append(re + im)
        return out

    def apply_pair(level, src, dst, v, half):
        vectors = [v, v + 1]
        for at_v, out in zip(vectors, hop_sums(src, vectors, half)):
            for pc in range(PC):
                value = out[pc]
                at = (pc // 3, pc % 3, at_v, half, pl.ds(FIRST, LAYERS), slice(None))
                if level == 1:
                    value = value - 36.0 * x_buf[at]
                if level == 3:
                    value = value * (1.0 / 162.0) + x_buf[at]
                dst[at] = value

    def correct_source(level, src, batch):
        correct(level - 1, src, batch)
        send_halo(level, src, batch)

    def correct_ahead(level, src, batch):
        ahead = batch + LEADS[level]

        @pl.when(ahead < BATCHES)
        def _():
            correct_source(level, src, ahead)

    def correct_first(level, src):
        def step(batch, carry):
            correct_source(level, src, batch)
            return carry

        lax.fori_loop(0, LEADS[level], step, 0)

    def batches(level, src, dst, first, last):
        def step(batch, carry):
            if level:
                correct_ahead(level, src, batch)

            def pair(i, inner):
                apply_pair(level, src, dst, batch * PER_BATCH + 2 * (i // HALVES), lax.rem(i, HALVES))
                return inner

            lax.fori_loop(0, PER_BATCH, pair, 0, unroll=PER_BATCH)
            return carry

        lax.fori_loop(first, last, step, 0)

    def first_halo(batch, carry):
        send_halo(0, x_buf, batch)
        return carry

    copies_in[0].wait()
    copies_in[2].wait()
    batches(0, x_buf, a_buf, 0, EARLY_BATCHES)
    pl.semaphore_wait(barrier, sum(len(ring) for ring in rings))
    top_copy.start()
    lax.fori_loop(0, BATCHES, first_halo, 0)
    tell(met_sem.at[0], rings[0])
    batches(0, x_buf, a_buf, EARLY_BATCHES, BATCHES)
    top_copy.wait_recv()
    lax.fori_loop(0, 9, prepare_below_edge, 0)
    pl.semaphore_wait(met_sem.at[0], len(rings[0]))
    tell(met_sem.at[1], rings[1])
    batches(1, a_buf, b_buf, 0, BATCHES)
    pl.semaphore_wait(met_sem.at[1], len(rings[1]))
    tell(met_sem.at[2], rings[2])
    correct_first(2, b_buf)
    batches(2, b_buf, a_buf, 0, BATCHES)
    correct_first(3, a_buf)

    result_rows = flat(b_buf)
    local_t = lax.rem(me_t, 8)

    def block_copy(tm_of):
        return pltpu.make_async_remote_copy(
            blocks.at[tm_of],
            got_ref.at[local_t, me_s],
            block_send_sem.at[tm_of],
            block_recv_sem.at[local_t * 4 + me_s],
            device_id=(tm_of, target_space),
            device_id_type=pl.DeviceIdType.MESH,
        )

    own_copy = pltpu.make_async_copy(blocks.at[me_t], got_ref.at[local_t, me_s], own_sem)

    def destination(half, i):
        dx, dz = STEPS[i]
        return half * 16 + lax.rem(x_at + dx, 4) * 4 + lax.rem(z_at + dz, 4)

    def foreign(tm_of):
        return jnp.logical_not(jnp.logical_and(has_self, tm_of == me_t))

    def send_block(tm_of):
        @pl.when(foreign(tm_of))
        def _():
            block_copy(tm_of).start()

    def last_pass(half, start, stop):
        def step(batch, carry):
            if half == 0:
                correct_ahead(3, a_buf, batch)

            def pair(i, inner):
                apply_pair(3, a_buf, b_buf, batch * PER_BATCH + 2 * i, half)
                return inner

            lax.fori_loop(0, PER_BATCH // 2, pair, 0, unroll=PER_BATCH // 2)
            return carry

        lax.fori_loop(start, stop, step, 0)

    def last_corrections(batch, carry):
        correct(3, None, batch)
        return carry

    def release(half):
        for side in range(2):
            row = FIRST if side else LAST
            for pc in range(PC):
                at = pl.ds((pc * NVEC * HALVES + half) * ROWS + row, NVEC, stride=HALVES * ROWS)
                result_rows[at, :] = result_rows[at, :] + delta[side, pc, pl.ds(half, NVEC, stride=HALVES), :]

        def arrange(layer, carry):
            tiles = []
            for x in (layer, layer + 4):
                pieces = []
                for pc in range(PC):
                    base = (pc * NVEC * HALVES + half) * ROWS + FIRST + x
                    pieces.append(result_rows[pl.ds(base, NVEC, stride=HALVES * ROWS), :])
                tiles.append(pieces)
                blocks[half * 16:(half + 1) * 16, x] = jnp.concatenate(pieces[:4], axis=0).T.astype(BF16).reshape(16, 8, LANES)
                for c in range(3):
                    re, im = pieces[c].astype(BF16), pieces[3 + c].astype(BF16)
                    at = pl.ds(pl.multiple_of(x * 64, 64), 64)
                    first = c * 256 + half * LANES
                    turned[at, first:first + LANES] = jnp.concatenate([re, im], axis=0)
                    turned[at, 768 + first:768 + first + LANES] = jnp.concatenate([im, -re], axis=0)
            rest = jnp.concatenate(tiles[0][4:] + tiles[1][4:], axis=0)
            blocks[half * 16:(half + 1) * 16, 8 + layer] = rest.T.astype(BF16).reshape(16, 8, LANES)
            return carry

        lax.fori_loop(0, 4, arrange, 0)

        if half == 0:
            pl.semaphore_wait(met_sem.at[2], len(rings[2]))

        for i in range(16):
            send_block(destination(half, i))

    last_pass(0, 0, BATCHES)
    last_pass(1, 0, BEFORE_RELEASE)
    lax.fori_loop(0, BATCHES, last_corrections, 0)
    release(0)
    last_pass(1, BEFORE_RELEASE, BATCHES)
    release(1)

    @pl.when(has_self)
    def _():
        own_copy.start()

    stored_copy.wait()

    def part_copy(step):
        other = lax.rem(me_s + step, 4)
        return pltpu.make_async_remote_copy(
            part_send.at[step - 1],
            part_recv.at[step - 1],
            part_send_sem.at[step - 1],
            part_recv_sem.at[step - 1],
            device_id={"space": other},
            device_id_type=pl.DeviceIdType.MESH,
        )

    def correlate(owner):
        def block(j, carry):
            first = owner * 112 + j * STORE_BLOCK
            some = [stored[pl.ds(first, STORE_BLOCK), rc].reshape(STORE_BLOCK * LAYERS, 256) for rc in range(PC)]
            product[...] = lax.dot_general(
                turned[...], jnp.concatenate(some, axis=1), (((1,), (1,)), ((), ())), preferred_element_type=F32
            )
            layer = lax.broadcasted_iota(jnp.int32, (64, STORE_BLOCK * LAYERS), 1) % LAYERS
            total = product[0:64]
            for x in range(1, LAYERS):
                total = jnp.where(layer == x, product[x * 64:(x + 1) * 64], total)
            diagonal[j, :, :STORE_BLOCK * LAYERS] = total
            return carry

        lax.fori_loop(0, 4, block, 0)
        values = jnp.concatenate([diagonal[j] for j in range(4)], axis=1)
        high = values.astype(BF16)
        low = (values - high.astype(F32)).astype(BF16)
        both = jnp.dot(jnp.concatenate([high, low], axis=0), ones[...], preferred_element_type=F32)
        return both[:64] + both[64:]

    def give(step, carry):
        part_send[step - 1] = correlate(lax.rem(me_s + step, 4))
        part_copy(step).start()
        return carry

    lax.fori_loop(1, 4, give, 0)
    total = correlate(me_s)
    for step in range(1, 4):
        part_copy(step).wait_recv()
        total = total + part_recv[step - 1]
    corr_ref[...] = total[:, :112]

    def finish_halo(i, carry):
        for level in range(APPLICATIONS):
            for side in range(2):
                halo_copy(level, side, i).wait_send()
        return carry

    lax.fori_loop(0, BATCHES, finish_halo, 0)
    top_copy.wait_send()
    for step in range(1, 4):
        part_copy(step).wait_send()

    @pl.when(has_self)
    def _():
        own_copy.wait()

    def finish_block(tm_of):
        @pl.when(foreign(tm_of))
        def _():
            block_copy(tm_of).wait_send()

    for half in range(HALVES):
        for i in range(16):
            finish_block(destination(half, i))

    def take_block(i, carry):
        tm_of = source_first + i // 4
        space_of = lax.rem(i, 4)

        @pl.when(jnp.logical_not(jnp.logical_and(tm_of == me_t, space_of == me_s)))
        def _():
            pltpu.make_async_remote_copy(
                blocks.at[0],
                got_ref.at[i // 4, space_of],
                block_send_sem.at[0],
                block_recv_sem.at[i],
                device_id=(tm_of, space_of),
                device_id_type=pl.DeviceIdType.MESH,
            ).wait_recv()

        return carry

    lax.fori_loop(0, 32, take_block, 0)


def unpack(corr_ref, got_ref, corr_out, solver_out):
    corr_out[...] = corr_ref[...]
    for t in range(4):
        for s in range(4):
            solver_out[t, s * 8:(s + 1) * 8, :, :LANES] = got_ref[t, s, 0:8]
            rest = got_ref[t, s, 8:12]
            solver_out[t, s * 8:s * 8 + 4, :, LANES:] = rest[:, :, :64]
            solver_out[t, s * 8 + 4:s * 8 + 8, :, LANES:] = rest[:, :, 64:]


def shards(start_block, gauge_links, stored_vectors):
    any_space = pl.BlockSpec(memory_space=pl.ANY)
    buffer = pltpu.VMEM((2, 3, NVEC, HALVES, ROWS, LANES), F32)
    halo = pltpu.VMEM((APPLICATIONS, 2, BATCHES, HALO_ROWS, LANES), BF16)
    halo_sem = pltpu.SemaphoreType.DMA((APPLICATIONS, 2, BATCHES))
    corr, got = pl.pallas_call(
        kernel,
        out_shape=(
            jax.ShapeDtypeStruct((64, 112), F32),
            jax.ShapeDtypeStruct((8, 4, 12, 8, LANES), BF16),
        ),
        in_specs=[any_space] * 3,
        out_specs=(pl.BlockSpec(memory_space=pltpu.VMEM), any_space),
        scratch_shapes=[
            buffer, buffer, buffer,
            pltpu.VMEM((3, 2, 9, HALVES, ROWS, LANES), F32),
            pltpu.VMEM((6, 9, 3, HALVES, LAYERS, LANES), F32),
            pltpu.VMEM((2, 9, 3, LAYERS, LANES), F32),
            pltpu.VMEM((36, LANES), F32),
            pltpu.VMEM((36, LANES), F32),
            halo, halo,
            pltpu.VMEM((448, 6, LAYERS, 256), BF16),
            pltpu.VMEM((32, 12, 8, LANES), BF16),
            pltpu.VMEM((512, 1536), BF16),
            pltpu.VMEM((512, STORE_BLOCK * LAYERS), F32),
            pltpu.VMEM((4, 64, 256), F32),
            pltpu.VMEM((1024, LANES), BF16),
            pltpu.VMEM((2, PC, NVEC * HALVES, LANES), F32),
            pltpu.VMEM((3, 64, LANES), F32),
            pltpu.VMEM((3, 64, LANES), F32),
            pltpu.SemaphoreType.DMA((4,)),
            pltpu.SemaphoreType.DMA,
            pltpu.SemaphoreType.DMA((2,)),
            halo_sem, halo_sem,
            pltpu.SemaphoreType.DMA((32,)),
            pltpu.SemaphoreType.DMA((32,)),
            pltpu.SemaphoreType.DMA,
            pltpu.SemaphoreType.DMA((3,)),
            pltpu.SemaphoreType.DMA((3,)),
            pltpu.SemaphoreType.REGULAR((3,)),
        ],
        compiler_params=pltpu.CompilerParams(
            collective_id=0, has_side_effects=True, vmem_limit_bytes=60 * 1024 * 1024
        ),
    )(
        start_block[0],
        gauge_links[0].reshape(3, 2, 9, LAYERS, 256),
        stored_vectors[0].reshape(448, 6, LAYERS, 256),
    )
    corr, solver = pl.pallas_call(
        unpack,
        grid=(2,),
        out_shape=(
            jax.ShapeDtypeStruct((64, 112), F32),
            jax.ShapeDtypeStruct((8, 32, 8, 192), BF16),
        ),
        in_specs=[
            pl.BlockSpec((64, 112), lambda i: (0, 0)),
            pl.BlockSpec((4, 4, 12, 8, LANES), lambda i: (i, 0, 0, 0, 0)),
        ],
        out_specs=(
            pl.BlockSpec((64, 112), lambda i: (0, 0)),
            pl.BlockSpec((4, 32, 8, 192), lambda i: (i, 0, 0, 0)),
        ),
    )(corr, got)
    return corr.T[None], solver


def solution(mesh):
    in_specs = (
        P("tm", None, None, None, "space", None),
        P("tm", None, None, None, None, "space", None),
        P("tm", None, None, None, "space", None),
    )
    out_specs = (P("tm", "space", None), P("space", None, "tm", None))
    return jax.shard_map(shards, mesh=mesh, in_specs=in_specs, out_specs=out_specs, check_vma=False)
```

```python
import jax
import jax.numpy as jnp
from jax import lax
from jax.experimental import pallas as pl
from jax.experimental.pallas import tpu as pltpu
from jax.sharding import PartitionSpec as P

F32 = jnp.float32
BF16 = jnp.bfloat16

NVEC = 32
LZ = 16
LAYERS = 8
HALVES = 2
LANES = 128
PC = 6
ROWS = 24
FIRST = 8
LAST = 15
BELOW = 7
ABOVE = 16
BATCHES = 8
PER_BATCH = NVEC // BATCHES
HALO_ROWS = PC * PER_BATCH * HALVES
APPLICATIONS = 4
STORE_BLOCK = 28
EARLY_BATCHES = 2
LEADS = (0, 0, 4, 8)
BEFORE_RELEASE = 2
STEPS = tuple(
    sorted(((dx, dz) for dx in range(4) for dz in range(4)), key=lambda d: (-sum(min(a, 4 - a) for a in d), d))
)


def lane_index():
    return lax.broadcasted_iota(jnp.int32, (LAYERS, LANES), 1)


def y_forward(own, other):
    keep = lane_index() < LANES - LZ
    return jnp.where(keep, pltpu.roll(own, LANES - LZ, 1), pltpu.roll(other, LANES - LZ, 1))


def y_backward(own, other):
    keep = lane_index() >= LZ
    return jnp.where(keep, pltpu.roll(own, LZ, 1), pltpu.roll(other, LZ, 1))


def z_forward(tile):
    along_z = lane_index() % LZ
    return jnp.where(along_z == LZ - 1, pltpu.roll(tile, LZ - 1, 1), pltpu.roll(tile, LANES - 1, 1))


def z_backward(tile):
    along_z = lane_index() % LZ
    return jnp.where(along_z == 0, pltpu.roll(tile, LANES - LZ + 1, 1), pltpu.roll(tile, 1, 1))


def kernel(
    start_ref, links_ref, stored_ref, corr_ref, got_ref,
    x_buf, a_buf, b_buf, raw, coef, edge, top_send, top_recv, halo_send, halo_recv,
    stored, blocks, turned, product, diagonal, ones, delta, part_send, part_recv,
    in_sem, stored_sem, top_sem, halo_send_sem, halo_recv_sem,
    block_send_sem, block_recv_sem, own_sem, part_send_sem, part_recv_sem, met_sem,
):
    me_t = lax.axis_index("tm")
    me_s = lax.axis_index("space")
    up = lax.rem(me_s + 1, 4)
    down = lax.rem(me_s + 3, 4)
    target_space = me_t // 8
    source_first = me_s * 8
    has_self = target_space == me_s

    copies_in = []
    for h in range(HALVES):
        lanes = pl.ds(h * LANES, LANES)
        copies_in.append(pltpu.make_async_copy(
            start_ref.at[:, :, :, :, lanes],
            x_buf.at[:, :, :, h, pl.ds(FIRST, LAYERS), :],
            in_sem.at[h],
        ))
        copies_in.append(pltpu.make_async_copy(
            links_ref.at[:, :, :, :, lanes],
            raw.at[:, :, :, h, pl.ds(FIRST, LAYERS), :],
            in_sem.at[2 + h],
        ))
    for copy in copies_in:
        copy.start()
    stored_copy = pltpu.make_async_copy(stored_ref, stored, stored_sem)
    stored_copy.start()

    y_lo, x_at, z_at = me_t // 16, lax.rem(me_t // 4, 4), lax.rem(me_t, 4)

    def x_partner(step):
        return (y_lo * 16 + lax.rem(x_at + step, 4) * 4 + z_at, me_s)

    def z_partner(step):
        return (y_lo * 16 + x_at * 4 + lax.rem(z_at + step, 4), me_s)

    def y_partner(step):
        return (lax.rem(y_lo + step // 4, 2) * 16 + x_at * 4 + z_at, lax.rem(me_s + step, 4))

    rings = ([x_partner(i) for i in range(1, 4)], [z_partner(i) for i in range(1, 4)], [y_partner(i) for i in range(1, 8)])

    def tell(sem, ring):
        for partner in ring:
            pl.semaphore_signal(sem, inc=1, device_id=partner, device_id_type=pl.DeviceIdType.MESH)

    barrier = pltpu.get_barrier_semaphore()
    for ring in rings:
        tell(barrier, ring)

    def flat(buf):
        return buf.reshape(PC * NVEC * HALVES * ROWS, LANES)

    raw_rows = raw.reshape(54 * HALVES * ROWS, LANES)
    zeros = jnp.zeros((LAYERS, LANES), F32)

    def clear(i, carry):
        for buf in (x_buf, a_buf, b_buf):
            for row in (BELOW, ABOVE):
                flat(buf)[pl.ds(i * LAYERS * ROWS + row, LAYERS, stride=ROWS), :] = zeros
        return carry

    lax.fori_loop(0, PC * NVEC * HALVES // LAYERS, clear, 0)
    column = lax.broadcasted_iota(jnp.int32, (1024, LANES), 0)
    group = jnp.where(column % 256 < STORE_BLOCK * LAYERS, column // 256 * STORE_BLOCK + column % 256 // LAYERS, -1)
    ones[...] = jnp.where(group == lax.broadcasted_iota(jnp.int32, (1024, LANES), 1), 1.0, 0.0).astype(BF16)
    diagonal[...] = jnp.zeros_like(diagonal)
    for i in range(5):
        raw_rows[pl.ds(min(i * LAYERS, 28) * ROWS + BELOW, LAYERS, stride=ROWS), :] = zeros

    copies_in[1].wait()
    copies_in[3].wait()

    top_send[...] = raw_rows[pl.ds(LAST, 36, stride=ROWS), :]

    top_copy = pltpu.make_async_remote_copy(
        top_send, top_recv, top_sem.at[0], top_sem.at[1],
        device_id={"space": up}, device_id_type=pl.DeviceIdType.MESH,
    )

    def halo_copy(level, side, batch):
        return pltpu.make_async_remote_copy(
            halo_send.at[level, side, batch],
            halo_recv.at[level, side, batch],
            halo_send_sem.at[level, side, batch],
            halo_recv_sem.at[level, side, batch],
            device_id={"space": up if side else down},
            device_id_type=pl.DeviceIdType.MESH,
        )

    def send_halo(level, buf, batch):
        rows = flat(buf)
        for side in range(2):
            row = LAST if side else FIRST
            pieces = []
            for pc in range(PC):
                base = ((pc * NVEC + batch * PER_BATCH) * HALVES) * ROWS + row
                pieces.append(rows[pl.ds(base, PER_BATCH * HALVES, stride=ROWS), :])
            halo_send[level, side, batch] = jnp.concatenate(pieces, axis=0).astype(BF16)
            halo_copy(level, side, batch).start()

    def put(direction, entry, half, re, im):
        coef[direction, entry, 0, half] = re
        coef[direction, entry, 1, half] = im - re
        coef[direction, entry, 2, half] = re + im

    def centre(d, part, entry, half):
        return raw[d, part, entry, half, FIRST:FIRST + LAYERS, :]

    def prepare(entry, carry):
        mirrored = lax.rem(entry, 3) * 3 + entry // 3
        for d in range(3):
            for half in range(HALVES):
                put(2 * d, entry, half, centre(d, 0, entry, half), centre(d, 1, entry, half))
        for half in range(HALVES):
            re, im = [y_backward(centre(1, part, entry, half), centre(1, part, entry, 1 - half)) for part in range(2)]
            put(3, mirrored, half, re, -im)
            put(5, mirrored, half, z_backward(centre(2, 0, entry, half)), -z_backward(centre(2, 1, entry, half)))
        return carry

    lax.fori_loop(0, 9, prepare, 0)

    def prepare_below(entry, carry):
        mirrored = lax.rem(entry, 3) * 3 + entry // 3
        for half in range(HALVES):
            re = raw[0, 0, entry, half, pl.ds(BELOW, LAYERS), :]
            im = raw[0, 1, entry, half, pl.ds(BELOW, LAYERS), :]
            put(1, mirrored, half, re, -im)
        return carry

    lax.fori_loop(0, 9, prepare_below, 0)

    edge_rows = coef.reshape(6 * 9 * 3 * HALVES * LAYERS, LANES)
    half_of = lax.broadcasted_iota(jnp.int32, (LAYERS, LANES), 0) % HALVES

    def alternate(rows, first, step):
        low = jnp.broadcast_to(rows[pl.ds(first, 1), :], (LAYERS, LANES))
        high = jnp.broadcast_to(rows[pl.ds(first + step, 1), :], (LAYERS, LANES))
        return jnp.where(half_of == 0, low, high)

    def prepare_above_edge(entry, carry):
        for kind in range(3):
            edge[0, entry, kind] = alternate(edge_rows, (entry * 3 + kind) * HALVES * LAYERS + LAYERS - 1, LAYERS)
        return carry

    lax.fori_loop(0, 9, prepare_above_edge, 0)

    def prepare_below_edge(entry, carry):
        mirrored = lax.rem(entry, 3) * 3 + entry // 3
        re = alternate(top_recv, entry * HALVES, 1)
        im = -alternate(top_recv, (9 + entry) * HALVES, 1)
        edge[1, mirrored, 0] = re
        edge[1, mirrored, 1] = im - re
        edge[1, mirrored, 2] = re + im
        return carry

    def correct(level, buf, batch):
        for side in range(2):
            halo_copy(level, side, batch).wait_recv()
            row = FIRST if side else LAST
            values = halo_recv[level, side, batch].astype(F32)
            count = PER_BATCH * HALVES
            parts = [values[pc * count:(pc + 1) * count] for pc in range(PC)]
            both = [parts[c] + parts[3 + c] for c in range(3)]
            for r in range(3):
                s = [None] * 3
                for c in range(3):
                    for kind, value in enumerate((both[c], parts[c], parts[3 + c])):
                        term = edge[side, r * 3 + c, kind] * value
                        s[kind] = term if s[kind] is None else s[kind] + term
                for pc, change in ((r, s[0] - s[2]), (3 + r, s[0] + s[1])):
                    if level == 3:
                        delta[side, pc, pl.ds(pl.multiple_of(batch * count, count), count), :] = change * (1.0 / 162.0)
                    else:
                        rows = flat(buf)
                        at = pl.ds(((pc * NVEC + batch * PER_BATCH) * HALVES) * ROWS + row, count, stride=ROWS)
                        rows[at, :] = rows[at, :] + change

    def hop_sums(src, vectors, half):
        sums = [[None] * 9 for _ in vectors]

        def add(direction, parts_of):
            for row in range(3):
                for col in range(3):
                    for kind in range(3):
                        factor = coef[direction, row * 3 + col, kind, half]
                        at = row * 3 + kind
                        for i, parts in enumerate(parts_of):
                            term = factor * parts[((6, 0, 3)[kind]) + col]
                            sums[i][at] = term if sums[i][at] is None else sums[i][at] + term

        def extended(parts):
            return parts + [parts[c] + parts[3 + c] for c in range(3)]

        def tiles(v, half_of, first):
            return [src[pc // 3, pc % 3, v, half_of, pl.ds(first, LAYERS), :] for pc in range(PC)]

        own = [tiles(v, half, FIRST) for v in vectors]
        other = [tiles(v, 1 - half, FIRST) for v in vectors]
        add(0, [extended(tiles(v, half, FIRST + 1)) for v in vectors])
        add(1, [extended(tiles(v, half, FIRST - 1)) for v in vectors])
        for direction, shift in ((2, y_forward), (3, y_backward)):
            add(direction, [extended([shift(a, b) for a, b in zip(mine, theirs)]) for mine, theirs in zip(own, other)])
        for direction, shift in ((4, z_forward), (5, z_backward)):
            add(direction, [extended([shift(a) for a in mine]) for mine in own])
        out = []
        for s, mine in zip(sums, own):
            re = [s[3 * r] - s[3 * r + 2] + 0.5 * mine[r] for r in range(3)]
            im = [s[3 * r] + s[3 * r + 1] + 0.5 * mine[3 + r] for r in range(3)]
            out.append(re + im)
        return out

    def apply_pair(level, src, dst, v, half):
        vectors = [v, v + 1]
        for at_v, out in zip(vectors, hop_sums(src, vectors, half)):
            for pc in range(PC):
                value = out[pc]
                at = (pc // 3, pc % 3, at_v, half, pl.ds(FIRST, LAYERS), slice(None))
                if level == 1:
                    value = value - 36.0 * x_buf[at]
                if level == 3:
                    value = value * (1.0 / 162.0) + x_buf[at]
                dst[at] = value

    def correct_source(level, src, batch):
        correct(level - 1, src, batch)
        send_halo(level, src, batch)

    def correct_ahead(level, src, batch):
        ahead = batch + LEADS[level]

        @pl.when(ahead < BATCHES)
        def _():
            correct_source(level, src, ahead)

    def correct_first(level, src):
        def step(batch, carry):
            correct_source(level, src, batch)
            return carry

        lax.fori_loop(0, LEADS[level], step, 0)

    def batches(level, src, dst, first, last):
        def step(batch, carry):
            if level:
                correct_ahead(level, src, batch)

            def pair(i, inner):
                apply_pair(level, src, dst, batch * PER_BATCH + 2 * (i // HALVES), lax.rem(i, HALVES))
                return inner

            lax.fori_loop(0, PER_BATCH, pair, 0, unroll=PER_BATCH)
            return carry

        lax.fori_loop(first, last, step, 0)

    def first_halo(batch, carry):
        send_halo(0, x_buf, batch)
        return carry

    copies_in[0].wait()
    copies_in[2].wait()
    batches(0, x_buf, a_buf, 0, EARLY_BATCHES)
    pl.semaphore_wait(barrier, sum(len(ring) for ring in rings))
    top_copy.start()
    lax.fori_loop(0, BATCHES, first_halo, 0)
    tell(met_sem.at[0], rings[0])
    batches(0, x_buf, a_buf, EARLY_BATCHES, BATCHES)
    top_copy.wait_recv()
    lax.fori_loop(0, 9, prepare_below_edge, 0)
    pl.semaphore_wait(met_sem.at[0], len(rings[0]))
    tell(met_sem.at[1], rings[1])
    batches(1, a_buf, b_buf, 0, BATCHES)
    pl.semaphore_wait(met_sem.at[1], len(rings[1]))
    tell(met_sem.at[2], rings[2])
    correct_first(2, b_buf)
    batches(2, b_buf, a_buf, 0, BATCHES)
    correct_first(3, a_buf)

    result_rows = flat(b_buf)
    local_t = lax.rem(me_t, 8)

    def block_copy(tm_of):
        return pltpu.make_async_remote_copy(
            blocks.at[tm_of],
            got_ref.at[local_t, me_s],
            block_send_sem.at[tm_of],
            block_recv_sem.at[local_t * 4 + me_s],
            device_id=(tm_of, target_space),
            device_id_type=pl.DeviceIdType.MESH,
        )

    own_copy = pltpu.make_async_copy(blocks.at[me_t], got_ref.at[local_t, me_s], own_sem)

    def destination(half, i):
        dx, dz = STEPS[i]
        return half * 16 + lax.rem(x_at + dx, 4) * 4 + lax.rem(z_at + dz, 4)

    def foreign(tm_of):
        return jnp.logical_not(jnp.logical_and(has_self, tm_of == me_t))

    def send_block(tm_of):
        @pl.when(foreign(tm_of))
        def _():
            block_copy(tm_of).start()

    def last_pass(half, start, stop):
        def step(batch, carry):
            if half == 0:
                correct_ahead(3, a_buf, batch)

            def pair(i, inner):
                apply_pair(3, a_buf, b_buf, batch * PER_BATCH + 2 * i, half)
                return inner

            lax.fori_loop(0, PER_BATCH // 2, pair, 0, unroll=PER_BATCH // 2)
            return carry

        lax.fori_loop(start, stop, step, 0)

    def last_corrections(batch, carry):
        correct(3, None, batch)
        return carry

    def release(half):
        for side in range(2):
            row = FIRST if side else LAST
            for pc in range(PC):
                at = pl.ds((pc * NVEC * HALVES + half) * ROWS + row, NVEC, stride=HALVES * ROWS)
                result_rows[at, :] = result_rows[at, :] + delta[side, pc, pl.ds(half, NVEC, stride=HALVES), :]

        def arrange(layer, carry):
            tiles = []
            for x in (layer, layer + 4):
                pieces = []
                for pc in range(PC):
                    base = (pc * NVEC * HALVES + half) * ROWS + FIRST + x
                    pieces.append(result_rows[pl.ds(base, NVEC, stride=HALVES * ROWS), :])
                tiles.append(pieces)
                blocks[half * 16:(half + 1) * 16, x] = jnp.concatenate(pieces[:4], axis=0).T.astype(BF16).reshape(16, 8, LANES)
                for c in range(3):
                    re, im = pieces[c].astype(BF16), pieces[3 + c].astype(BF16)
                    at = pl.ds(pl.multiple_of(x * 64, 64), 64)
                    first = c * 256 + half * LANES
                    turned[at, first:first + LANES] = jnp.concatenate([re, im], axis=0)
                    turned[at, 768 + first:768 + first + LANES] = jnp.concatenate([im, -re], axis=0)
            rest = jnp.concatenate(tiles[0][4:] + tiles[1][4:], axis=0)
            blocks[half * 16:(half + 1) * 16, 8 + layer] = rest.T.astype(BF16).reshape(16, 8, LANES)
            return carry

        lax.fori_loop(0, 4, arrange, 0)

        if half == 0:
            pl.semaphore_wait(met_sem.at[2], len(rings[2]))

        for i in range(16):
            send_block(destination(half, i))

    last_pass(0, 0, BATCHES)
    last_pass(1, 0, BEFORE_RELEASE)
    lax.fori_loop(0, BATCHES, last_corrections, 0)
    release(0)
    last_pass(1, BEFORE_RELEASE, BATCHES)
    release(1)

    @pl.when(has_self)
    def _():
        own_copy.start()

    stored_copy.wait()

    def part_copy(step):
        other = lax.rem(me_s + step, 4)
        return pltpu.make_async_remote_copy(
            part_send.at[step - 1],
            part_recv.at[step - 1],
            part_send_sem.at[step - 1],
            part_recv_sem.at[step - 1],
            device_id={"space": other},
            device_id_type=pl.DeviceIdType.MESH,
        )

    def correlate(owner):
        def block(j, carry):
            first = owner * 112 + j * STORE_BLOCK
            some = [stored[pl.ds(first, STORE_BLOCK), rc].reshape(STORE_BLOCK * LAYERS, 256) for rc in range(PC)]
            product[...] = lax.dot_general(
                turned[...], jnp.concatenate(some, axis=1), (((1,), (1,)), ((), ())), preferred_element_type=F32
            )
            layer = lax.broadcasted_iota(jnp.int32, (64, STORE_BLOCK * LAYERS), 1) % LAYERS
            total = product[0:64]
            for x in range(1, LAYERS):
                total = jnp.where(layer == x, product[x * 64:(x + 1) * 64], total)
            diagonal[j, :, :STORE_BLOCK * LAYERS] = total
            return carry

        lax.fori_loop(0, 4, block, 0)
        values = jnp.concatenate([diagonal[j] for j in range(4)], axis=1)
        high = values.astype(BF16)
        low = (values - high.astype(F32)).astype(BF16)
        both = jnp.dot(jnp.concatenate([high, low], axis=0), ones[...], preferred_element_type=F32)
        return both[:64] + both[64:]

    def give(step, carry):
        part_send[step - 1] = correlate(lax.rem(me_s + step, 4))
        part_copy(step).start()
        return carry

    lax.fori_loop(1, 4, give, 0)
    total = correlate(me_s)

    def finish_halo(i, carry):
        for level in range(APPLICATIONS):
            for side in range(2):
                halo_copy(level, side, i).wait_send()
        return carry

    lax.fori_loop(0, BATCHES, finish_halo, 0)
    top_copy.wait_send()
    for step in range(1, 4):
        part_copy(step).wait_send()

    @pl.when(has_self)
    def _():
        own_copy.wait()

    def finish_block(tm_of):
        @pl.when(foreign(tm_of))
        def _():
            block_copy(tm_of).wait_send()

    for half in range(HALVES):
        for i in range(16):
            finish_block(destination(half, i))

    for step in range(1, 4):
        part_copy(step).wait_recv()
        total = total + part_recv[step - 1]
    corr_ref[...] = total[:, :112]

    def take_block(i, carry):
        tm_of = source_first + i // 4
        space_of = lax.rem(i, 4)

        @pl.when(jnp.logical_not(jnp.logical_and(tm_of == me_t, space_of == me_s)))
        def _():
            pltpu.make_async_remote_copy(
                blocks.at[0],
                got_ref.at[i // 4, space_of],
                block_send_sem.at[0],
                block_recv_sem.at[i],
                device_id=(tm_of, space_of),
                device_id_type=pl.DeviceIdType.MESH,
            ).wait_recv()

        return carry

    lax.fori_loop(0, 32, take_block, 0)


def unpack(corr_ref, got_ref, corr_out, solver_out):
    corr_out[...] = corr_ref[...]
    for t in range(4):
        for s in range(4):
            solver_out[t, s * 8:(s + 1) * 8, :, :LANES] = got_ref[t, s, 0:8]
            rest = got_ref[t, s, 8:12]
            solver_out[t, s * 8:s * 8 + 4, :, LANES:] = rest[:, :, :64]
            solver_out[t, s * 8 + 4:s * 8 + 8, :, LANES:] = rest[:, :, 64:]


def shards(start_block, gauge_links, stored_vectors):
    any_space = pl.BlockSpec(memory_space=pl.ANY)
    buffer = pltpu.VMEM((2, 3, NVEC, HALVES, ROWS, LANES), F32)
    halo = pltpu.VMEM((APPLICATIONS, 2, BATCHES, HALO_ROWS, LANES), BF16)
    halo_sem = pltpu.SemaphoreType.DMA((APPLICATIONS, 2, BATCHES))
    corr, got = pl.pallas_call(
        kernel,
        out_shape=(
            jax.ShapeDtypeStruct((64, 112), F32),
            jax.ShapeDtypeStruct((8, 4, 12, 8, LANES), BF16),
        ),
        in_specs=[any_space] * 3,
        out_specs=(pl.BlockSpec(memory_space=pltpu.VMEM), any_space),
        scratch_shapes=[
            buffer, buffer, buffer,
            pltpu.VMEM((3, 2, 9, HALVES, ROWS, LANES), F32),
            pltpu.VMEM((6, 9, 3, HALVES, LAYERS, LANES), F32),
            pltpu.VMEM((2, 9, 3, LAYERS, LANES), F32),
            pltpu.VMEM((36, LANES), F32),
            pltpu.VMEM((36, LANES), F32),
            halo, halo,
            pltpu.VMEM((448, 6, LAYERS, 256), BF16),
            pltpu.VMEM((32, 12, 8, LANES), BF16),
            pltpu.VMEM((512, 1536), BF16),
            pltpu.VMEM((512, STORE_BLOCK * LAYERS), F32),
            pltpu.VMEM((4, 64, 256), F32),
            pltpu.VMEM((1024, LANES), BF16),
            pltpu.VMEM((2, PC, NVEC * HALVES, LANES), F32),
            pltpu.VMEM((3, 64, LANES), F32),
            pltpu.VMEM((3, 64, LANES), F32),
            pltpu.SemaphoreType.DMA((4,)),
            pltpu.SemaphoreType.DMA,
            pltpu.SemaphoreType.DMA((2,)),
            halo_sem, halo_sem,
            pltpu.SemaphoreType.DMA((32,)),
            pltpu.SemaphoreType.DMA((32,)),
            pltpu.SemaphoreType.DMA,
            pltpu.SemaphoreType.DMA((3,)),
            pltpu.SemaphoreType.DMA((3,)),
            pltpu.SemaphoreType.REGULAR((3,)),
        ],
        compiler_params=pltpu.CompilerParams(
            collective_id=0, has_side_effects=True, vmem_limit_bytes=60 * 1024 * 1024
        ),
    )(
        start_block[0],
        gauge_links[0].reshape(3, 2, 9, LAYERS, 256),
        stored_vectors[0].reshape(448, 6, LAYERS, 256),
    )
    corr, solver = pl.pallas_call(
        unpack,
        grid=(2,),
        out_shape=(
            jax.ShapeDtypeStruct((64, 112), F32),
            jax.ShapeDtypeStruct((8, 32, 8, 192), BF16),
        ),
        in_specs=[
            pl.BlockSpec((64, 112), lambda i: (0, 0)),
            pl.BlockSpec((4, 4, 12, 8, LANES), lambda i: (i, 0, 0, 0, 0)),
        ],
        out_specs=(
            pl.BlockSpec((64, 112), lambda i: (0, 0)),
            pl.BlockSpec((4, 32, 8, 192), lambda i: (i, 0, 0, 0)),
        ),
    )(corr, got)
    return corr.T[None], solver


def solution(mesh):
    in_specs = (
        P("tm", None, None, None, "space", None),
        P("tm", None, None, None, None, "space", None),
        P("tm", None, None, None, "space", None),
    )
    out_specs = (P("tm", "space", None), P("space", None, "tm", None))
    return jax.shard_map(shards, mesh=mesh, in_specs=in_specs, out_specs=out_specs, check_vma=False)
```
